8 devices in a mesh: dp: 1 (over z), pool: 2 (over y), ep: 4 (over x, core).
Axes of the slice: x: 2, y: 2, z: 1, core: 2. Of those that a mesh axis runs over, the one named last changes fastest.
Arguments:
- hidden: bfloat16 [128, 1024], P(('dp', 'ep'))
- k_cache: bfloat16 [2, 128, 128, 2, 128], P(None, ('dp', 'ep'))
- v_cache: bfloat16 [2, 128, 128, 2, 128], P(None, ('dp', 'ep'))
- lengths: int32 [128], P(('dp', 'ep'))
- expert_ids: int32 [2, 128, 8], P(None, ('dp', 'ep'))
- w_query: bfloat16 [2, 1024, 2048], replicated
- w_key: bfloat16 [2, 1024, 256], replicated
- w_value: bfloat16 [2, 1024, 256], replicated
- w_out: bfloat16 [2, 2048, 1024], replicated
- w_router: float32 [2, 1024, 64], replicated
- w_gate: bfloat16 [2, 64, 1024, 768], P(None, 'ep')
- w_up: bfloat16 [2, 64, 1024, 768], P(None, 'ep')
- w_down: bfloat16 [2, 64, 768, 1024], P(None, 'ep')
Outputs:
- output: bfloat16 [128, 1024], P(('dp', 'ep'))
All inputs are finite; a program needn't handle non-finite values.
Results may differ from the reference program's by a relative error of at most 0.0178775.
Values are sent between devices in bfloat16 or wider.
A program may use at most 1 GiB of HBM per device.

```python
import math
import jax
import jax.numpy as jnp
from jax import lax

LAYERS = 2
D = 1024
FF = 768
EXPERTS = 64
TOPK = 8
HEADS = 16
KV_HEADS = 2
HEAD = 128
TOK = 32
SEQ = 128
NATT = 4
CAP = 12

EPSILON = 1e-6
ROPE_BASE = 10000.0


def draw_routing(key):
    total = TOK * TOPK
    layers_ids = []
    for layer in range(LAYERS):
        key_hot, key_dev = jax.random.split(jax.random.fold_in(key, layer))
        order = jax.random.permutation(key_hot, EXPERTS)
        n_hot = layer + 1
        n_cold = EXPERTS - n_hot
        spare = total - n_hot * CAP
        base_count = spare // n_cold
        extra_count = spare % n_cold

        def one_block(block_key):
            key_rank, key_tok = jax.random.split(block_key)
            ranks = jax.random.permutation(key_rank, n_cold)
            cold_counts = base_count + (ranks < extra_count).astype(jnp.int32)
            counts = jnp.zeros((EXPERTS,), jnp.int32).at[order[:n_hot]].set(CAP).at[order[n_hot:]].set(cold_counts)
            bounds = jnp.cumsum(counts)
            flat = jnp.sum((bounds[None, :] <= jnp.arange(total)[:, None]).astype(jnp.int32), axis=1)
            table = flat.reshape(TOPK, TOK).T
            return table[jax.random.permutation(key_tok, TOK)]

        block_ids = jax.vmap(one_block)(jax.random.split(key_dev, NATT))
        layers_ids.append(block_ids.reshape(NATT * TOK, TOPK))
    return jnp.stack(layers_ids)


def draw_lengths(key):
    tok_total = NATT * TOK
    key_exp, key_len, key_full = jax.random.split(key, 3)
    top_exp = int(math.log2(SEQ))
    exponent = jax.random.randint(key_exp, (tok_total,), 0, top_exp + 1)
    span = jnp.left_shift(jnp.ones((tok_total,), jnp.int32), exponent)
    lens = 1 + jax.random.randint(key_len, (tok_total,), 0, span)
    return lens.at[jax.random.randint(key_full, (), 0, tok_total)].set(SEQ)


def setup_inputs(seed: int = 0, part: int = 0) -> dict:
    tok_total = NATT * TOK
    base_key = jax.random.key(seed)
    part_key = jax.random.fold_in(jax.random.key(seed + 1), part)
    key_hid, key_kc, key_vc, key_len, key_ids = jax.random.split(part_key, 5)
    keys_w = jax.random.split(base_key, 8)

    def gauss(key, shape, scale):
        return jax.random.normal(key, shape, jnp.float32) * scale

    return {
        "hidden": gauss(key_hid, (tok_total, D), 1.0).astype(jnp.bfloat16),
        "k_cache": gauss(key_kc, (LAYERS, tok_total, SEQ, KV_HEADS, HEAD), 1.0).astype(jnp.bfloat16),
        "v_cache": gauss(key_vc, (LAYERS, tok_total, SEQ, KV_HEADS, HEAD), 1.0).astype(jnp.bfloat16),
        "lengths": draw_lengths(key_len),
        "expert_ids": draw_routing(key_ids),
        "w_query": gauss(keys_w[0], (LAYERS, D, HEADS * HEAD), 1.5 * D ** -0.5).astype(jnp.bfloat16),
        "w_key": gauss(keys_w[1], (LAYERS, D, KV_HEADS * HEAD), D ** -0.5).astype(jnp.bfloat16),
        "w_value": gauss(keys_w[2], (LAYERS, D, KV_HEADS * HEAD), D ** -0.5).astype(jnp.bfloat16),
        "w_out": gauss(keys_w[3], (LAYERS, HEADS * HEAD, D), 2.0 * (HEADS * HEAD) ** -0.5).astype(jnp.bfloat16),
        "w_router": gauss(keys_w[4], (LAYERS, D, EXPERTS), 1.5 * D ** -0.5),
        "w_gate": gauss(keys_w[5], (LAYERS, EXPERTS, D, FF), D ** -0.5).astype(jnp.bfloat16),
        "w_up": gauss(keys_w[6], (LAYERS, EXPERTS, D, FF), D ** -0.5).astype(jnp.bfloat16),
        "w_down": gauss(keys_w[7], (LAYERS, EXPERTS, FF, D), 2.0 * FF ** -0.5).astype(jnp.bfloat16),
    }


def rms_normed(values):
    return values * lax.rsqrt(jnp.mean(values * values, axis=-1, keepdims=True) + EPSILON)


def rotary(vectors, positions):
    half = vectors.shape[-1] // 2
    freqs = ROPE_BASE ** (-2.0 * jnp.arange(half, dtype=jnp.float32) / vectors.shape[-1])
    angle = positions[:, None, None] * freqs[None, None, :]
    cosine = jnp.cos(angle)
    sine = jnp.sin(angle)
    first = vectors[..., :half]
    second = vectors[..., half:]
    return jnp.concatenate([first * cosine - second * sine, second * cosine + first * sine], axis=-1)


def attend_block(hidden_blk, keys_blk, vals_blk, lens_blk, w_q, w_k, w_v, w_o):
    hidden_f = hidden_blk.astype(jnp.float32)
    normed = rms_normed(hidden_f).astype(jnp.bfloat16)
    positions = lens_blk.astype(jnp.float32)
    query = rotary(jnp.dot(normed, w_q, preferred_element_type=jnp.float32).reshape(TOK, HEADS, HEAD), positions)
    query = query.astype(jnp.bfloat16).reshape(TOK, KV_HEADS, HEADS // KV_HEADS, HEAD).astype(jnp.float32)
    key_new = rotary(jnp.dot(normed, w_k, preferred_element_type=jnp.float32).reshape(TOK, KV_HEADS, HEAD), positions)
    key_new = key_new.astype(jnp.bfloat16).astype(jnp.float32)
    val_new = jnp.dot(normed, w_v, preferred_element_type=jnp.float32).astype(jnp.bfloat16).reshape(TOK, KV_HEADS, HEAD)
    scale = HEAD ** -0.5
    scores = jnp.einsum("tkgd,tskd->tkgs", query, keys_blk.astype(jnp.float32)) * scale
    valid = jnp.arange(SEQ)[None, None, None, :] < lens_blk[:, None, None, None]
    scores = jnp.where(valid, scores, -jnp.inf)
    score_new = jnp.einsum("tkgd,tkd->tkg", query, key_new) * scale
    peak = jnp.maximum(jnp.max(scores, axis=-1), score_new)
    weights = jnp.exp(scores - peak[..., None])
    weight_new = jnp.exp(score_new - peak)
    denominator = jnp.sum(weights, axis=-1) + weight_new
    mixed = jnp.einsum("tkgs,tskd->tkgd", weights.astype(jnp.bfloat16).astype(jnp.float32), vals_blk.astype(jnp.float32))
    mixed = mixed + weight_new.astype(jnp.bfloat16).astype(jnp.float32)[..., None] * val_new.astype(jnp.float32)[:, :, None, :]
    attended = (mixed / denominator[..., None]).astype(jnp.bfloat16).reshape(TOK, HEADS * HEAD)
    return (hidden_f + jnp.dot(attended, w_o, preferred_element_type=jnp.float32)).astype(jnp.bfloat16)


def moe_layer(attn_out, ids_layer, w_r, w_gate, w_up, w_down):
    residual = attn_out.astype(jnp.float32)
    mixed_in = rms_normed(residual).astype(jnp.bfloat16)
    logits = jnp.dot(mixed_in.astype(jnp.float32), w_r)
    gates = jax.nn.softmax(jnp.take_along_axis(logits, ids_layer, axis=1), axis=-1)
    blocks_in = mixed_in.reshape(NATT, TOK, D).astype(jnp.float32)
    id_blocks = ids_layer.reshape(NATT, TOK, TOPK)
    gate_blocks = gates.reshape(NATT, TOK, TOPK)
    slot_ids = jnp.arange(CAP)

    def step(total_acc, layer_pack):
        expert, w_one, w_three, w_two = layer_pack
        hit = id_blocks == expert
        weight = jnp.sum(jnp.where(hit, gate_blocks, 0.0), axis=2)
        chosen = jnp.any(hit, axis=2)
        rank = jnp.cumsum(chosen.astype(jnp.int32), axis=1) - 1
        select = ((rank[:, None, :] == slot_ids[None, :, None]) & chosen[:, None, :]).astype(jnp.float32)
        rows = jnp.einsum("bct,btd->bcd", select, blocks_in).astype(jnp.bfloat16).reshape(NATT * CAP, D)
        inner = jax.nn.silu(jnp.dot(rows, w_one, preferred_element_type=jnp.float32)) * jnp.dot(rows, w_three, preferred_element_type=jnp.float32)
        result = jnp.dot(inner.astype(jnp.bfloat16), w_two, preferred_element_type=jnp.float32).astype(jnp.bfloat16)
        back = jnp.einsum("bct,bcd->btd", select, result.reshape(NATT, CAP, D).astype(jnp.float32))
        return total_acc + weight[:, :, None] * back, None

    total_acc, _ = lax.scan(step, jnp.zeros((NATT, TOK, D), jnp.float32), (jnp.arange(EXPERTS), w_gate, w_up, w_down))
    return (residual + total_acc.reshape(NATT * TOK, D)).astype(jnp.bfloat16)


def reference(hidden, k_cache, v_cache, lengths, expert_ids, w_query, w_key, w_value, w_out, w_router, w_gate, w_up, w_down):
    def layer_step(state, layer_pack):
        cache_k, cache_v, ids_layer, w_q, w_k, w_v, w_o, w_r, w_one, w_three, w_two = layer_pack

        def per_block(block_in):
            return attend_block(block_in[0], block_in[1], block_in[2], block_in[3], w_q, w_k, w_v, w_o)

        attn_out = lax.map(per_block, (state.reshape(NATT, TOK, D), cache_k.reshape(NATT, TOK, SEQ, KV_HEADS, HEAD), cache_v.reshape(NATT, TOK, SEQ, KV_HEADS, HEAD), lengths.reshape(NATT, TOK)))
        return moe_layer(attn_out.reshape(NATT * TOK, D), ids_layer, w_r, w_one, w_three, w_two), None

    final, _ = lax.scan(layer_step, hidden, (k_cache, v_cache, expert_ids, w_query, w_key, w_value, w_out, w_router, w_gate, w_up, w_down))
    return final
```

```python
import functools
import math

import jax
import jax.numpy as jnp
from jax import lax
from jax.experimental import pallas as pl
from jax.experimental.pallas import tpu as pltpu
from jax.sharding import PartitionSpec as P

EPSILON = 1e-6
ROPE_BASE = 10000.0
MESH = pl.DeviceIdType.MESH
F32 = jnp.float32
BF16 = jnp.bfloat16
NT = (((1,), (1,)), ((), ()))


def rms_normed(values):
    return values * lax.rsqrt(jnp.mean(values * values, axis=-1, keepdims=True) + EPSILON)


def kernel(cfg, hid, kc, vc, lens, ids, wq, wk, wv, wo, wr, wg, wu, wd, out,
           wq_s, wk_s, wv_s, wo_s, wr_s, kb, vb, w1_s, w3_s, w2_s,
           x_s, a_s, ids_s, idt_s, q_s, s_s, o_s,
           u_all, g_all, gb_s, inner_s, part, rbuf, xfin,
           sem_a, sem_w, sem_w2, sem_u, sem_us, sem_g, sem_gs, sem_c, sem_cs, sem_x, sem_out):
    layers, n_pool, n_ep, tok, heads, kvh, hd, seq, n_loc, ff, model = cfg
    n_dev = n_pool * n_ep
    n_chunk, _, _, cw = w2_s.shape
    p = lax.axis_index("pool")
    ep = lax.axis_index("ep")
    me = p * n_ep + ep
    row0 = pl.multiple_of(p * tok, tok)

    def peer(j):
        d = lax.rem(me + j, n_dev)
        return d, {"pool": d // n_ep, "ep": lax.rem(d, n_ep)}

    barrier = pltpu.get_barrier_semaphore()
    for j in range(1, n_dev):
        pl.semaphore_signal(barrier, inc=1, device_id=peer(j)[1], device_id_type=MESH)

    def attn_copy(l, k):
        src, dst = [
            (lambda: wq.at[l], wq_s), (lambda: wk.at[l], wk_s), (lambda: wv.at[l], wv_s),
            (lambda: kc.at[l, pl.ds(row0, tok)], kb), (lambda: vc.at[l, pl.ds(row0, tok)], vb),
            (lambda: wo.at[l], wo_s), (lambda: wr.at[l], wr_s),
        ][k]
        return pltpu.make_async_copy(src(), dst, sem_a.at[k])

    def up_copies(l, i):
        e = p * n_loc + i
        return [
            pltpu.make_async_copy(wg.at[l, e], w1_s.at[i], sem_w.at[0, i]),
            pltpu.make_async_copy(wu.at[l, e], w3_s.at[i], sem_w.at[1, i]),
        ]

    def down_copy(l, n):
        return pltpu.make_async_copy(
            wd.at[l, pl.ds(p * n_loc, n_loc), :, pl.ds(n * cw, cw)], w2_s.at[n], sem_w2.at[n])

    hid_copy = pltpu.make_async_copy(hid.at[pl.ds(row0, tok)], xfin.at[0], sem_a.at[7])
    ids_copy = pltpu.make_async_copy(ids, ids_s, sem_a.at[8])
    hid_copy.start()
    ids_copy.start()
    for k in range(7):
        attn_copy(0, k).start()
    for i in range(n_loc):
        for c in up_copies(0, i):
            c.start()
    for n in range(n_chunk):
        down_copy(0, n).start()

    rows = lax.broadcasted_iota(jnp.int32, (tok, hd), 0)
    lanes = lax.broadcasted_iota(jnp.int32, (tok, hd), 1)
    len_i = jnp.zeros((tok, hd), jnp.int32)
    for t in range(tok):
        len_i = jnp.where(rows == t, lens[p * tok + t], len_i)
    half = hd // 2
    pair = jnp.where(lanes < half, lanes, lanes - half).astype(F32)
    freq = jnp.exp(pair * (-2.0 * math.log(ROPE_BASE) / hd))
    angle = len_i.astype(F32) * freq
    cosine = jnp.cos(angle)
    sine = jnp.sin(angle)
    sine = jnp.where(lanes < half, -sine, sine)

    def rotary(v):
        return v * cosine + pltpu.roll(v, half, 1) * sine

    ids_copy.wait()
    for l in range(layers):
        idf = jnp.concatenate([ids_s[l].astype(F32), jnp.zeros((ids_s.shape[1], 128 - ids_s.shape[2]), F32)], axis=1)
        idt_s[l] = jnp.transpose(idf)
    hid_copy.wait()
    x_s[...] = xfin[0].astype(F32)

    scale = hd ** -0.5
    group = heads // kvh

    def attention(l):
        x = x_s[...]
        h = rms_normed(x).astype(BF16)
        attn_copy(l, 0).wait()
        qc = 256
        for c in range(heads * hd // qc):
            qq = jnp.dot(h, wq_s[:, c * qc:(c + 1) * qc], preferred_element_type=F32)
            for s in range(qc // hd):
                hh = c * (qc // hd) + s
                q_s[hh * tok:(hh + 1) * tok, :] = rotary(qq[:, s * hd:(s + 1) * hd]).astype(BF16).astype(F32)
        attn_copy(l, 1).wait()
        kk = jnp.dot(h, wk_s[...], preferred_element_type=F32)
        k_new = [rotary(kk[:, s * hd:(s + 1) * hd]).astype(BF16).astype(F32) for s in range(kvh)]
        attn_copy(l, 2).wait()
        vv = jnp.dot(h, wv_s[...], preferred_element_type=F32).astype(BF16).astype(F32)
        v_new = [vv[:, s * hd:(s + 1) * hd] for s in range(kvh)]
        attn_copy(l, 3).wait()
        for t in range(tok):
            qt = q_s[pl.ds(t, heads, stride=tok), :].astype(BF16)
            st = lax.dot_general(qt, kb[t], NT, preferred_element_type=F32) * scale
            for b in range(kvh * seq // 128):
                s_s[b, pl.ds(t, heads, stride=tok), :] = st[:, b * 128:(b + 1) * 128]
        lane = lax.broadcasted_iota(jnp.int32, (tok, 128), 1)
        w_new = []
        den = []
        for hh in range(heads):
            kv = hh // group
            sl = slice(hh * tok, (hh + 1) * tok)
            sn = jnp.sum(q_s[sl, :] * k_new[kv], axis=-1, keepdims=True) * scale
            blocks = []
            for b in range(kvh * seq // 128):
                col = lane + b * 128
                ok = (lax.rem(col, kvh) == kv) & (col // kvh < len_i)
                blocks.append(jnp.where(ok, s_s[b, sl, :], -jnp.inf))
            top = functools.reduce(jnp.maximum, blocks)
            peak = jnp.maximum(jnp.max(top, axis=-1, keepdims=True), sn)
            ws = [jnp.exp(v - peak) for v in blocks]
            for b, w in enumerate(ws):
                s_s[b, sl, :] = w
            wn = jnp.exp(sn - peak)
            w_new.append(wn)
            den.append(jnp.sum(functools.reduce(jnp.add, ws), axis=-1, keepdims=True) + wn)
        attn_copy(l, 4).wait()
        for t in range(tok):
            pt = jnp.concatenate(
                [s_s[b, pl.ds(t, heads, stride=tok), :] for b in range(kvh * seq // 128)], axis=1).astype(BF16)
            o_s[pl.ds(t, heads, stride=tok), :] = jnp.dot(pt, vb[t], preferred_element_type=F32)
        pieces = []
        for hh in range(heads):
            sl = slice(hh * tok, (hh + 1) * tok)
            mixed = o_s[sl, :] + w_new[hh].astype(BF16).astype(F32) * v_new[hh // group]
            pieces.append((mixed / den[hh]).astype(BF16))
        o = jnp.concatenate(pieces, axis=1)
        attn_copy(l, 5).wait()
        oc = 256
        for c in range(model // oc):
            sl = slice(c * oc, (c + 1) * oc)
            a_s[:, sl] = (x[:, sl] + jnp.dot(o, wo_s[:, sl], preferred_element_type=F32)).astype(BF16).astype(F32)

    def u_copy(l, j, src):
        d, dev = peer(j)
        return pltpu.make_async_remote_copy(
            src_ref=u_all.at[l, src], dst_ref=u_all.at[l, src], send_sem=sem_us.at[l, j], recv_sem=sem_u.at[l, src],
            device_id=dev, device_id_type=MESH)

    def g_copy(l, j, src):
        d, dev = peer(j)
        return pltpu.make_async_remote_copy(
            src_ref=g_all.at[l, src], dst_ref=g_all.at[l, src], send_sem=sem_gs.at[l, j], recv_sem=sem_g.at[l, src],
            device_id=dev, device_id_type=MESH)

    def c_copy(l, n, j, src):
        d, dev = peer(j)
        return pltpu.make_async_remote_copy(
            src_ref=part.at[l, n, d], dst_ref=rbuf.at[l, n, src], send_sem=sem_cs.at[l, n, j], recv_sem=sem_c.at[l, n, src],
            device_id=dev, device_id_type=MESH)

    def route(l):
        u = rms_normed(a_s[...]).astype(BF16)
        u_all[l, me] = u
        for j in range(1, n_dev):
            u_copy(l, j, me).start()
        attn_copy(l, 6).wait()
        rest = wr_s[...]
        n_exp = rest.shape[0]
        logits = jnp.zeros((tok, n_exp), F32)
        for _ in range(3):
            piece = rest.astype(BF16)
            rest = rest - piece.astype(F32)
            logits = logits + lax.dot_general(u, piece, NT, preferred_element_type=F32)
        mine = idt_s[l, pl.ds(row0, tok), :]
        expert = lax.broadcasted_iota(jnp.int32, (tok, n_exp), 1).astype(F32)
        chosen = jnp.zeros((tok, n_exp), jnp.bool_)
        for k in range(mine.shape[1]):
            chosen = chosen | (mine[:, k:k + 1] == expert)
        masked = jnp.where(chosen, logits, -jnp.inf)
        w = jnp.exp(masked - jnp.max(masked, axis=-1, keepdims=True))
        gates = w / jnp.sum(w, axis=-1, keepdims=True)
        g_all[l, me] = jnp.concatenate([gates, jnp.zeros((tok, 128 - n_exp), F32)], axis=1)
        for j in range(1, n_dev):
            g_copy(l, j, me).start()

    def experts(l):
        for j in range(1, n_dev):
            u_copy(l, j, peer(j)[0]).wait_recv()
        n_tok = n_dev * tok

        def up_step(i, carry):
            for c in up_copies(l, i):
                c.wait()
            ub = u_all[l].reshape(n_tok, model)
            fc = 256
            for n in range(ff // fc):
                sl = slice(n * fc, (n + 1) * fc)
                one = jnp.dot(ub, w1_s[i, :, sl], preferred_element_type=F32)
                three = jnp.dot(ub, w3_s[i, :, sl], preferred_element_type=F32)
                inner_s[i, :, sl] = (jax.nn.silu(one) * three).astype(BF16)
            if l + 1 < layers:
                for c in up_copies(l + 1, i):
                    c.start()
            return carry

        lax.fori_loop(0, n_loc, up_step, 0)
        for j in range(1, n_dev):
            g_copy(l, j, peer(j)[0]).wait_recv()
        gates = g_all[l].reshape(n_tok, 128)
        lane = lax.broadcasted_iota(jnp.int32, (n_tok, 128), 1)
        first = (ep * n_pool + p) * n_loc
        for i in range(n_loc):
            g = jnp.sum(jnp.where(lane == first + i, gates, 0.0), axis=-1, keepdims=True)
            gb_s[i] = jnp.broadcast_to(g, (n_tok, 128))

        def down_step(n, carry):
            down_copy(l, n).wait()
            acc = [jnp.zeros((n_tok, 128), F32) for _ in range(cw // 128)]
            for i in range(n_loc):
                y = jnp.dot(inner_s[i], w2_s[n, i], preferred_element_type=F32).astype(BF16).astype(F32)
                g = gb_s[i]
                for b in range(cw // 128):
                    acc[b] = acc[b] + jnp.where(g > 0.0, g * y[:, b * 128:(b + 1) * 128], 0.0)
            for b in range(cw // 128):
                part[l, n, :, :, b * 128:(b + 1) * 128] = acc[b].reshape(n_dev, tok, 128)
            for j in range(1, n_dev):
                c_copy(l, n, j, me).start()
            if l + 1 < layers:
                down_copy(l + 1, n).start()
            return carry

        lax.fori_loop(0, n_chunk, down_step, 0)

    other = 1 - p

    def x_copy(n):
        return pltpu.make_async_remote_copy(
            src_ref=xfin.at[p, :, pl.ds(n * cw, cw)], dst_ref=xfin.at[p, :, pl.ds(n * cw, cw)],
            send_sem=sem_x.at[0, n], recv_sem=sem_x.at[1, n],
            device_id={"pool": other, "ep": ep}, device_id_type=MESH)

    def x_arrival(n):
        return pltpu.make_async_remote_copy(
            src_ref=xfin.at[other, :, pl.ds(n * cw, cw)], dst_ref=xfin.at[other, :, pl.ds(n * cw, cw)],
            send_sem=sem_x.at[0, n], recv_sem=sem_x.at[1, n],
            device_id={"pool": other, "ep": ep}, device_id_type=MESH)

    def combine(l):
        for n in range(n_chunk):
            total = part[l, n, me]
            for j in range(1, n_dev):
                src = peer(j)[0]
                c_copy(l, n, j, src).wait_recv()
                total = total + rbuf[l, n, src]
            sl = slice(n * cw, (n + 1) * cw)
            x = (a_s[:, sl] + total).astype(BF16)
            if l + 1 < layers:
                x_s[:, sl] = x.astype(F32)
            else:
                xfin[p, :, sl] = x
                x_copy(n).start()

    for l in range(layers):
        attention(l)
        if l == 0:
            pl.semaphore_wait(barrier, n_dev - 1)
        route(l)
        if l + 1 < layers:
            for k in range(7):
                attn_copy(l + 1, k).start()
        experts(l)
        combine(l)

    own = pltpu.make_async_copy(xfin.at[p], out.at[pl.ds(row0, tok)], sem_out.at[0])
    own.start()
    for n in range(n_chunk):
        x_arrival(n).wait_recv()
    partner = pltpu.make_async_copy(xfin.at[other], out.at[pl.ds(pl.multiple_of(other * tok, tok), tok)], sem_out.at[1])
    partner.start()
    for n in range(n_chunk):
        x_copy(n).wait_send()
    for l in range(layers):
        for j in range(1, n_dev):
            u_copy(l, j, me).wait_send()
            g_copy(l, j, me).wait_send()
            for n in range(n_chunk):
                c_copy(l, n, j, me).wait_send()
    own.wait()
    partner.wait()


def solution(mesh):
    n_pool = mesh.shape["pool"]
    n_ep = mesh.shape["ep"]
    n_dev = n_pool * n_ep

    def body(hidden, k_cache, v_cache, lengths, expert_ids, w_query, w_key, w_value, w_out, w_router, w_gate, w_up, w_down):
        layers, n_tok, seq, kvh, hd = k_cache.shape
        tok = n_tok // n_pool
        model = hidden.shape[1]
        heads = w_query.shape[2] // hd
        n_loc = w_gate.shape[1] // n_pool
        ff = w_gate.shape[3]
        n_exp = w_router.shape[2]
        topk = expert_ids.shape[2]
        cw = 256
        n_chunk = model // cw
        kflat = k_cache.reshape(layers, n_tok, seq * kvh, hd)
        vflat = v_cache.reshape(layers, n_tok, seq * kvh, hd)
        ids = jnp.swapaxes(expert_ids, 1, 2)
        router = jnp.swapaxes(w_router, 1, 2)
        cfg = (layers, n_pool, n_ep, tok, heads, kvh, hd, seq, n_loc, ff, model)
        any_spec = pl.BlockSpec(memory_space=pl.ANY)
        smem_spec = pl.BlockSpec(memory_space=pltpu.SMEM)
        vm = pltpu.VMEM
        dma = pltpu.SemaphoreType.DMA
        return pl.pallas_call(
            functools.partial(kernel, cfg),
            out_shape=jax.ShapeDtypeStruct((n_tok, model), BF16),
            in_specs=[any_spec] * 3 + [smem_spec] + [any_spec] * 9,
            out_specs=any_spec,
            scratch_shapes=[
                vm((model, heads * hd), BF16), vm((model, kvh * hd), BF16), vm((model, kvh * hd), BF16),
                vm((heads * hd, model), BF16), vm((n_exp, model), F32),
                vm((tok, seq * kvh, hd), BF16), vm((tok, seq * kvh, hd), BF16),
                vm((n_loc, model, ff), BF16), vm((n_loc, model, ff), BF16), vm((n_chunk, n_loc, ff, cw), BF16),
                vm((tok, model), F32), vm((tok, model), F32), vm((layers, topk, n_tok), jnp.int32), vm((layers, 128, topk), F32),
                vm((heads * tok, hd), F32), vm((kvh * seq // 128, heads * tok, 128), F32), vm((heads * tok, hd), F32),
                vm((layers, n_dev, tok, model), BF16), vm((layers, n_dev, tok, 128), F32), vm((n_loc, n_dev * tok, 128), F32),
                vm((n_loc, n_dev * tok, ff), BF16), vm((layers, n_chunk, n_dev, tok, cw), F32),
                vm((layers, n_chunk, n_dev, tok, cw), F32), vm((n_pool, tok, model), BF16),
                dma((9,)), dma((2, n_loc)), dma((n_chunk,)), dma((layers, n_dev)), dma((layers, n_dev)),
                dma((layers, n_dev)), dma((layers, n_dev)), dma((layers, n_chunk, n_dev)), dma((layers, n_chunk, n_dev)),
                dma((2, n_chunk)), dma((2,)),
            ],
            compiler_params=pltpu.CompilerParams(
                collective_id=0, has_side_effects=True, vmem_limit_bytes=66 * 1024 * 1024 - 2 * 1024 * 1024 - 65536),
        )(hidden, kflat, vflat, lengths, ids, w_query, w_key, w_value, w_out, router, w_gate, w_up, w_down)

    rows_spec = ("dp", "ep")
    in_specs = (P(rows_spec, None), P(None, rows_spec), P(None, rows_spec), P(rows_spec), P(None, rows_spec, None), P(), P(), P(), P(), P(), P(None, "ep"), P(None, "ep"), P(None, "ep"))
    return jax.shard_map(body, mesh=mesh, in_specs=in_specs, out_specs=P(rows_spec, None), check_vma=False)
```

```python
import functools
import math

import jax
import jax.numpy as jnp
from jax import lax
from jax.experimental import pallas as pl
from jax.experimental.pallas import tpu as pltpu
from jax.sharding import PartitionSpec as P

EPSILON = 1e-6
ROPE_BASE = 10000.0
MESH = pl.DeviceIdType.MESH
F32 = jnp.float32
BF16 = jnp.bfloat16
NT = (((1,), (1,)), ((), ()))


def rms_normed(values):
    return values * lax.rsqrt(jnp.mean(values * values, axis=-1, keepdims=True) + EPSILON)


def kernel(cfg, hid, kc, vc, lens, ids, wq, wk, wv, wo, wr, wg, wu, wd, xfin,
           wq_s, wk_s, wv_s, wo_s, wr_s, kb, vb, w1_s, w3_s, w2_s,
           x_s, a_s, ids_s, idt_s, q_s, s_s, o_s,
           u_all, g_all, gb_s, inner_s, part, sbuf, red, rbuf, hid_s,
           sem_a, sem_w, sem_w2, sem_u, sem_us, sem_g, sem_gs, sem_d, sem_ds, sem_c, sem_cs, sem_x):
    layers, n_pool, n_ep, tok, heads, kvh, hd, seq, n_loc, ff, model = cfg
    n_dev = n_pool * n_ep
    n_chunk, _, _, cw = w2_s.shape
    p = lax.axis_index("pool")
    ep = lax.axis_index("ep")
    me = p * n_ep + ep
    row0 = pl.multiple_of(p * tok, tok)

    cx = ep // 2
    cc = lax.rem(ep, 2)

    def peer(dy, dx, dc):
        y, e = lax.rem(p + dy, 2), lax.rem(cx + dx, 2) * 2 + lax.rem(cc + dc, 2)
        return y * n_ep + e, {"pool": y, "ep": e}

    others = [(1, 1, 1), (1, 1, 0), (0, 1, 1), (1, 0, 1), (0, 1, 0), (1, 0, 0), (0, 0, 1)]
    chips = [(0, 0), (0, 1), (1, 0), (1, 1)]

    barrier = pltpu.get_barrier_semaphore()
    for rel in others:
        pl.semaphore_signal(barrier, inc=1, device_id=peer(*rel)[1], device_id_type=MESH)

    def attn_copy(l, k):
        src, dst = [
            (lambda: wq.at[l], wq_s), (lambda: wk.at[l], wk_s), (lambda: wv.at[l], wv_s),
            (lambda: kc.at[l, pl.ds(row0, tok)], kb), (lambda: vc.at[l, pl.ds(row0, tok)], vb),
            (lambda: wo.at[l], wo_s), (lambda: wr.at[l], wr_s),
        ][k]
        return pltpu.make_async_copy(src(), dst, sem_a.at[k])

    def up_copies(l, i):
        e = p * n_loc + i
        return [
            pltpu.make_async_copy(wg.at[l, e], w1_s.at[i], sem_w.at[0, i]),
            pltpu.make_async_copy(wu.at[l, e], w3_s.at[i], sem_w.at[1, i]),
        ]

    def down_copy(l, n):
        return pltpu.make_async_copy(
            wd.at[l, pl.ds(p * n_loc, n_loc), :, pl.ds(n * cw, cw)], w2_s.at[n], sem_w2.at[n])

    hid_copy = pltpu.make_async_copy(hid.at[pl.ds(row0, tok)], hid_s, sem_a.at[7])
    ids_copy = pltpu.make_async_copy(ids, ids_s, sem_a.at[8])
    hid_copy.start()
    ids_copy.start()
    for k in range(7):
        attn_copy(0, k).start()

    def start_up(l, lo, hi):
        for i in range(lo, hi):
            for c in up_copies(l, i):
                c.start()

    rows = lax.broadcasted_iota(jnp.int32, (tok, hd), 0)
    lanes = lax.broadcasted_iota(jnp.int32, (tok, hd), 1)
    len_i = jnp.zeros((tok, hd), jnp.int32)
    for t in range(tok):
        len_i = jnp.where(rows == t, lens[p * tok + t], len_i)
    half = hd // 2
    pair = jnp.where(lanes < half, lanes, lanes - half).astype(F32)
    freq = jnp.exp(pair * (-2.0 * math.log(ROPE_BASE) / hd))
    angle = len_i.astype(F32) * freq
    cosine = jnp.cos(angle)
    sine = jnp.sin(angle)
    sine = jnp.where(lanes < half, -sine, sine)

    def rotary(v):
        return v * cosine + pltpu.roll(v, half, 1) * sine

    with jax.named_scope("idswait"):
        ids_copy.wait()
    for l in range(layers):
        idf = jnp.concatenate([ids_s[l].astype(F32), jnp.zeros((ids_s.shape[1], 128 - ids_s.shape[2]), F32)], axis=1)
        idt_s[l] = jnp.transpose(idf)
    with jax.named_scope("hidwait"):
        hid_copy.wait()
    x_s[...] = hid_s[...].astype(F32)

    scale = hd ** -0.5
    group = heads // kvh

    def attention(l):
        x = x_s[...]
        h = rms_normed(x).astype(BF16)
        with jax.named_scope(f"await0_{l}"):
            for k in range(3 if l == 0 else 7):
                attn_copy(l, k).wait()
        if l == 0:
            start_up(0, 0, 2)
        qc = 256
        for c in range(heads * hd // qc):
            qq = jnp.dot(h, wq_s[:, c * qc:(c + 1) * qc], preferred_element_type=F32)
            for s in range(qc // hd):
                hh = c * (qc // hd) + s
                q_s[hh * tok:(hh + 1) * tok, :] = rotary(qq[:, s * hd:(s + 1) * hd]).astype(BF16).astype(F32)
        kk = jnp.dot(h, wk_s[...], preferred_element_type=F32)
        k_new = [rotary(kk[:, s * hd:(s + 1) * hd]).astype(BF16).astype(F32) for s in range(kvh)]
        vv = jnp.dot(h, wv_s[...], preferred_element_type=F32).astype(BF16).astype(F32)
        v_new = [vv[:, s * hd:(s + 1) * hd] for s in range(kvh)]
        if l == 0:
            with jax.named_scope(f"await3_{l}"):
                attn_copy(l, 3).wait()
                attn_copy(l, 4).wait()
            start_up(0, 2, 4)
        for t in range(tok):
            qt = q_s[pl.ds(t, heads, stride=tok), :].astype(BF16)
            st = lax.dot_general(qt, kb[t], NT, preferred_element_type=F32) * scale
            for b in range(kvh * seq // 128):
                s_s[b, pl.ds(t, heads, stride=tok), :] = st[:, b * 128:(b + 1) * 128]
        lane = lax.broadcasted_iota(jnp.int32, (tok, 128), 1)
        w_new = []
        den = []
        for hh in range(heads):
            kv = hh // group
            sl = slice(hh * tok, (hh + 1) * tok)
            sn = jnp.sum(q_s[sl, :] * k_new[kv], axis=-1, keepdims=True) * scale
            blocks = []
            for b in range(kvh * seq // 128):
                col = lane + b * 128
                ok = (lax.rem(col, kvh) == kv) & (col // kvh < len_i)
                blocks.append(jnp.where(ok, s_s[b, sl, :], -jnp.inf))
            top = functools.reduce(jnp.maximum, blocks)
            peak = jnp.maximum(jnp.max(top, axis=-1, keepdims=True), sn)
            ws = [jnp.exp(v - peak) for v in blocks]
            for b, w in enumerate(ws):
                s_s[b, sl, :] = w
            wn = jnp.exp(sn - peak)
            w_new.append(wn)
            den.append(jnp.sum(functools.reduce(jnp.add, ws), axis=-1, keepdims=True) + wn)
        for t in range(tok):
            pt = jnp.concatenate(
                [s_s[b, pl.ds(t, heads, stride=tok), :] for b in range(kvh * seq // 128)], axis=1).astype(BF16)
            o_s[pl.ds(t, heads, stride=tok), :] = jnp.dot(pt, vb[t], preferred_element_type=F32)
        pieces = []
        for hh in range(heads):
            sl = slice(hh * tok, (hh + 1) * tok)
            mixed = o_s[sl, :] + w_new[hh].astype(BF16).astype(F32) * v_new[hh // group]
            pieces.append((mixed / den[hh]).astype(BF16))
        o = jnp.concatenate(pieces, axis=1)
        if l == 0:
            with jax.named_scope(f"await5_{l}"):
                attn_copy(l, 5).wait()
            start_up(0, 4, n_loc)
            for n in range(n_chunk):
                down_copy(0, n).start()
        oc = 256
        for c in range(model // oc):
            sl = slice(c * oc, (c + 1) * oc)
            a_s[:, sl] = (x[:, sl] + jnp.dot(o, wo_s[:, sl], preferred_element_type=F32)).astype(BF16).astype(F32)

    def u_copy(l, j, src):
        return pltpu.make_async_remote_copy(
            src_ref=u_all.at[l, src], dst_ref=u_all.at[l, src], send_sem=sem_us.at[l, j], recv_sem=sem_u.at[l, j],
            device_id=peer(*others[j])[1], device_id_type=MESH)

    def g_copy(l, j, src):
        return pltpu.make_async_remote_copy(
            src_ref=g_all.at[l, src], dst_ref=g_all.at[l, src], send_sem=sem_gs.at[l, j], recv_sem=sem_g.at[l, j],
            device_id=peer(*others[j])[1], device_id_type=MESH)

    def d_copy(l, n, k):
        dest = peer(0, 0, 1)[0] if k == 0 else peer(*chips[k], 0)[0]
        return pltpu.make_async_remote_copy(
            src_ref=part.at[l, n, dest], dst_ref=sbuf.at[l, n, k], send_sem=sem_ds.at[l, n, k], recv_sem=sem_d.at[l, n, k],
            device_id=peer(0, 0, 1)[1], device_id_type=MESH)

    def c_copy(l, n, k):
        return pltpu.make_async_remote_copy(
            src_ref=red.at[l, n, k], dst_ref=rbuf.at[l, n, k], send_sem=sem_cs.at[l, n, k], recv_sem=sem_c.at[l, n, k],
            device_id=peer(*chips[k], 1)[1], device_id_type=MESH)

    far_first = (3, 1, 2)

    def route(l):
        u = rms_normed(a_s[...]).astype(BF16)
        u_all[l, me] = u
        for j in range(len(others)):
            u_copy(l, j, me).start()
        if l == 0:
            with jax.named_scope(f"await6_{l}"):
                attn_copy(l, 6).wait()
        rest = wr_s[...]
        n_exp = rest.shape[0]
        logits = jnp.zeros((tok, n_exp), F32)
        for _ in range(3):
            piece = rest.astype(BF16)
            rest = rest - piece.astype(F32)
            logits = logits + lax.dot_general(u, piece, NT, preferred_element_type=F32)
        mine = idt_s[l, pl.ds(row0, tok), :]
        expert = lax.broadcasted_iota(jnp.int32, (tok, n_exp), 1).astype(F32)
        chosen = jnp.zeros((tok, n_exp), jnp.bool_)
        for k in range(mine.shape[1]):
            chosen = chosen | (mine[:, k:k + 1] == expert)
        masked = jnp.where(chosen, logits, -jnp.inf)
        w = jnp.exp(masked - jnp.max(masked, axis=-1, keepdims=True))
        gates = w / jnp.sum(w, axis=-1, keepdims=True)
        g_all[l, me] = jnp.concatenate([gates, jnp.zeros((tok, 128 - n_exp), F32)], axis=1)
        for j in range(len(others)):
            g_copy(l, j, me).start()

    n_tok = n_dev * tok
    fc = 256
    per = 4

    def up_block(l, g):
        with jax.named_scope(f"upwait{l}"):
            for i in range(g * per, (g + 1) * per):
                for c in up_copies(l, i):
                    c.wait()
        for i in range(g * per, (g + 1) * per):
            ub = u_all[l].reshape(n_tok, model)
            for n in range(ff // fc):
                sl = slice(n * fc, (n + 1) * fc)
                one = jnp.dot(ub, w1_s[i, :, sl], preferred_element_type=F32)
                three = jnp.dot(ub, w3_s[i, :, sl], preferred_element_type=F32)
                inner_s[i, :, sl] = (jax.nn.silu(one) * three).astype(BF16)

    def gate_columns(l):
        gates = g_all[l].reshape(n_tok, 128)
        lane = lax.broadcasted_iota(jnp.int32, (n_tok, 128), 1)
        first = (ep * n_pool + p) * n_loc
        for i in range(n_loc):
            g = jnp.sum(jnp.where(lane == first + i, gates, 0.0), axis=-1, keepdims=True)
            gb_s[i] = jnp.broadcast_to(g, (n_tok, 128))

    def down_block(l, n):
        acc = [jnp.zeros((n_tok, 128), F32) for _ in range(cw // 128)]
        for i in range(n_loc):
            y = jnp.dot(inner_s[i], w2_s[n, i], preferred_element_type=F32).astype(BF16).astype(F32)
            g = gb_s[i]
            for b in range(cw // 128):
                acc[b] = acc[b] + jnp.where(g > 0.0, g * y[:, b * 128:(b + 1) * 128], 0.0)
        for b in range(cw // 128):
            part[l, n, :, :, b * 128:(b + 1) * 128] = acc[b].reshape(n_dev, tok, 128)

    def forward_chunk(l, n):
        for k in far_first:
            d_copy(l, n, k).wait_recv()
            red[l, n, k] = part[l, n, peer(*chips[k], 1)[0]] + sbuf[l, n, k]
            c_copy(l, n, k).start()

    def experts(l):
        with jax.named_scope(f"uwait{l}"):
            for j in range(len(others)):
                u_copy(l, j, peer(*others[j])[0]).wait_recv()
        for g in range(n_loc // per):
            with jax.named_scope(f"up{l}"):
                up_block(l, g)
            if l + 1 < layers:
                start_up(l + 1, g * per, (g + 1) * per)
            if g == 0:
                with jax.named_scope(f"gwait{l}"):
                    for j in range(len(others)):
                        g_copy(l, j, peer(*others[j])[0]).wait_recv()
                gate_columns(l)
        for n in range(n_chunk):
            with jax.named_scope(f"downwait{l}"):
                down_copy(l, n).wait()
            with jax.named_scope(f"down{l}"):
                down_block(l, n)
            for k in far_first + (0,):
                d_copy(l, n, k).start()
            if l + 1 < layers:
                down_copy(l + 1, n).start()
            if n > 0:
                with jax.named_scope(f"fwd{l}"):
                    forward_chunk(l, n - 1)
        with jax.named_scope(f"fwd{l}"):
            forward_chunk(l, n_chunk - 1)

    other = 1 - p
    orow = pl.multiple_of(other * tok, tok)

    def x_copy(n, row):
        view = xfin.at[pl.ds(row, tok), pl.ds(n * cw, cw)]
        return pltpu.make_async_remote_copy(
            src_ref=view, dst_ref=view, send_sem=sem_x.at[0, n], recv_sem=sem_x.at[1, n],
            device_id={"pool": other, "ep": ep}, device_id_type=MESH)

    def combine(l):
        for n in range(n_chunk):
            d_copy(l, n, 0).wait_recv()
            total = part[l, n, me] + sbuf[l, n, 0]
            for k in far_first:
                c_copy(l, n, k).wait_recv()
                total = total + rbuf[l, n, k]
            sl = slice(n * cw, (n + 1) * cw)
            x = (a_s[:, sl] + total).astype(BF16)
            if l + 1 < layers:
                x_s[:, sl] = x.astype(F32)
            else:
                xfin[pl.ds(row0, tok), sl] = x
                x_copy(n, row0).start()

    for l in range(layers):
        with jax.named_scope(f"attention{l}"):
            attention(l)
        if l == 0:
            with jax.named_scope("barrier"):
                pl.semaphore_wait(barrier, len(others))
        with jax.named_scope(f"route{l}"):
            route(l)
        if l + 1 < layers:
            for k in range(7):
                attn_copy(l + 1, k).start()
        experts(l)
        with jax.named_scope(f"combine{l}"):
            combine(l)

    with jax.named_scope("xwait"):
        for n in range(n_chunk):
            x_copy(n, orow).wait_recv()
    with jax.named_scope("drain"):
        for n in range(n_chunk):
            x_copy(n, row0).wait_send()
        for l in range(layers):
            for j in range(len(others)):
                u_copy(l, j, me).wait_send()
                g_copy(l, j, me).wait_send()
            for n in range(n_chunk):
                for k in range(4):
                    d_copy(l, n, k).wait_send()
                    if k:
                        c_copy(l, n, k).wait_send()


def solution(mesh):
    n_pool = mesh.shape["pool"]
    n_ep = mesh.shape["ep"]
    n_dev = n_pool * n_ep

    def body(hidden, k_cache, v_cache, lengths, expert_ids, w_query, w_key, w_value, w_out, w_router, w_gate, w_up, w_down):
        layers, n_tok, seq, kvh, hd = k_cache.shape
        tok = n_tok // n_pool
        model = hidden.shape[1]
        heads = w_query.shape[2] // hd
        n_loc = w_gate.shape[1] // n_pool
        ff = w_gate.shape[3]
        n_exp = w_router.shape[2]
        topk = expert_ids.shape[2]
        cw = 256
        n_chunk = model // cw
        kflat = k_cache.reshape(layers, n_tok, seq * kvh, hd)
        vflat = v_cache.reshape(layers, n_tok, seq * kvh, hd)
        ids = jnp.swapaxes(expert_ids, 1, 2)
        router = jnp.swapaxes(w_router, 1, 2)
        cfg = (layers, n_pool, n_ep, tok, heads, kvh, hd, seq, n_loc, ff, model)
        any_spec = pl.BlockSpec(memory_space=pl.ANY)
        smem_spec = pl.BlockSpec(memory_space=pltpu.SMEM)
        vm = pltpu.VMEM
        dma = pltpu.SemaphoreType.DMA
        return pl.pallas_call(
            functools.partial(kernel, cfg),
            out_shape=vm((n_tok, model), BF16),
            in_specs=[any_spec] * 3 + [smem_spec] + [any_spec] * 9,
            out_specs=pl.BlockSpec(memory_space=pltpu.VMEM),
            scratch_shapes=[
                vm((model, heads * hd), BF16), vm((model, kvh * hd), BF16), vm((model, kvh * hd), BF16),
                vm((heads * hd, model), BF16), vm((n_exp, model), F32),
                vm((tok, seq * kvh, hd), BF16), vm((tok, seq * kvh, hd), BF16),
                vm((n_loc, model, ff), BF16), vm((n_loc, model, ff), BF16), vm((n_chunk, n_loc, ff, cw), BF16),
                vm((tok, model), F32), vm((tok, model), F32), vm((layers, topk, n_tok), jnp.int32), vm((layers, 128, topk), F32),
                vm((heads * tok, hd), F32), vm((kvh * seq // 128, heads * tok, 128), F32), vm((heads * tok, hd), F32),
                vm((layers, n_dev, tok, model), BF16), vm((layers, n_dev, tok, 128), F32), vm((n_loc, n_dev * tok, 128), F32),
                vm((n_loc, n_dev * tok, ff), BF16), vm((layers, n_chunk, n_dev, tok, cw), F32),
                vm((layers, n_chunk, 4, tok, cw), F32), vm((layers, n_chunk, 4, tok, cw), F32), vm((layers, n_chunk, 4, tok, cw), F32),
                vm((tok, model), BF16),
                dma((9,)), dma((2, n_loc)), dma((n_chunk,)), dma((layers, 7)), dma((layers, 7)), dma((layers, 7)), dma((layers, 7)),
                dma((layers, n_chunk, 4)), dma((layers, n_chunk, 4)), dma((layers, n_chunk, 4)), dma((layers, n_chunk, 4)), dma((2, n_chunk)),
            ],
            compiler_params=pltpu.CompilerParams(
                collective_id=0, has_side_effects=True, vmem_limit_bytes=63 * 1024 * 1024),
        )(hidden, kflat, vflat, lengths, ids, w_query, w_key, w_value, w_out, router, w_gate, w_up, w_down)

    rows_spec = ("dp", "ep")
    in_specs = (P(rows_spec, None), P(None, rows_spec), P(None, rows_spec), P(rows_spec), P(None, rows_spec, None), P(), P(), P(), P(), P(), P(None, "ep"), P(None, "ep"), P(None, "ep"))
    return jax.shard_map(body, mesh=mesh, in_specs=in_specs, out_specs=P(rows_spec, None), check_vma=False)
```

```python
import functools
import math

import jax
import jax.numpy as jnp
from jax import lax
from jax.experimental import pallas as pl
from jax.experimental.pallas import tpu as pltpu
from jax.sharding import PartitionSpec as P

EPSILON = 1e-6
ROPE_BASE = 10000.0
MESH = pl.DeviceIdType.MESH
F32 = jnp.float32
BF16 = jnp.bfloat16
NT = (((1,), (1,)), ((), ()))


def rms_normed(values):
    return values * lax.rsqrt(jnp.mean(values * values, axis=-1, keepdims=True) + EPSILON)


def kernel(cfg, hid, kc, vc, lens, ids, wq, wk, wv, wo, wr, wg, wu, wd, xfin,
           wq_s, wk_s, wv_s, wo_s, wr_s, kb, vb, w1_s, w3_s, w2_s,
           x_s, a_s, ids_s, idt_s, q_s, s_s, o_s,
           u_all, g_all, gb_s, inner_s, part, sbuf, red, rbuf, hid_s, lens_s,
           sem_a, sem_w, sem_w2, sem_u, sem_us, sem_g, sem_gs, sem_d, sem_ds, sem_c, sem_cs, sem_x):
    layers, n_pool, n_ep, tok, heads, kvh, hd, seq, n_loc, ff, model = cfg
    n_dev = n_pool * n_ep
    n_chunk, _, _, cw = w2_s.shape
    p = lax.axis_index("pool")
    ep = lax.axis_index("ep")
    me = p * n_ep + ep
    row0 = pl.multiple_of(p * tok, tok)

    cx = ep // 2
    cc = lax.rem(ep, 2)

    def peer(dy, dx, dc):
        y, e = lax.rem(p + dy, 2), lax.rem(cx + dx, 2) * 2 + lax.rem(cc + dc, 2)
        return y * n_ep + e, {"pool": y, "ep": e}

    others = [(1, 1, 1), (1, 1, 0), (0, 1, 1), (1, 0, 1), (0, 1, 0), (1, 0, 0), (0, 0, 1)]
    chips = [(0, 0), (0, 1), (1, 0), (1, 1)]

    def attn_copy(l, k):
        src, dst = [
            (lambda: wq.at[l], wq_s), (lambda: wk.at[l], wk_s), (lambda: wv.at[l], wv_s),
            (lambda: kc.at[l, pl.ds(row0, tok)], kb), (lambda: vc.at[l, pl.ds(row0, tok)], vb),
            (lambda: wo.at[l], wo_s), (lambda: wr.at[l], wr_s),
        ][k]
        return pltpu.make_async_copy(src(), dst, sem_a.at[k])

    def up_copies(l, g):
        e = p * n_loc + g * 2
        return [
            pltpu.make_async_copy(wg.at[l, pl.ds(e, 2)], w1_s.at[pl.ds(g * 2, 2)], sem_w.at[0, g]),
            pltpu.make_async_copy(wu.at[l, pl.ds(e, 2)], w3_s.at[pl.ds(g * 2, 2)], sem_w.at[1, g]),
        ]

    def start_up(l, g):
        for c in up_copies(l, g):
            c.start()

    def down_copy(l, n):
        return pltpu.make_async_copy(
            wd.at[l, pl.ds(p * n_loc, n_loc), :, pl.ds(n * cw, cw)], w2_s.at[n], sem_w2.at[n])

    hid_copy = pltpu.make_async_copy(hid.at[pl.ds(row0, tok)], hid_s, sem_a.at[7])
    ids_copy = pltpu.make_async_copy(ids, ids_s, sem_a.at[8])
    len_copy = pltpu.make_async_copy(lens, lens_s, sem_a.at[9])
    len_copy.start()
    hid_copy.start()
    ids_copy.start()
    for k in range(3):
        attn_copy(0, k).start()

    barrier = pltpu.get_barrier_semaphore()
    for rel in others:
        pl.semaphore_signal(barrier, inc=1, device_id=peer(*rel)[1], device_id_type=MESH)

    with jax.named_scope("lenwait"):
        len_copy.wait()
    rows = lax.broadcasted_iota(jnp.int32, (tok, hd), 0)
    lanes = lax.broadcasted_iota(jnp.int32, (tok, hd), 1)
    len_i = jnp.zeros((tok, hd), jnp.int32)
    for t in range(tok):
        len_i = jnp.where(rows == t, lens_s[p * tok + t], len_i)
    half = hd // 2
    pair = jnp.where(lanes < half, lanes, lanes - half).astype(F32)
    freq = jnp.exp(pair * (-2.0 * math.log(ROPE_BASE) / hd))
    angle = len_i.astype(F32) * freq
    cosine = jnp.cos(angle)
    sine = jnp.sin(angle)
    sine = jnp.where(lanes < half, -sine, sine)

    def rotary(v):
        return v * cosine + pltpu.roll(v, half, 1) * sine

    with jax.named_scope("idswait"):
        ids_copy.wait()
    for l in range(layers):
        idf = jnp.concatenate([ids_s[l].astype(F32), jnp.zeros((ids_s.shape[1], 128 - ids_s.shape[2]), F32)], axis=1)
        idt_s[l] = jnp.transpose(idf)
    for k in range(3, 7):
        attn_copy(0, k).start()
    with jax.named_scope("hidwait"):
        hid_copy.wait()
    x_s[...] = hid_s[...].astype(F32)

    scale = hd ** -0.5
    group = heads // kvh

    def attention(l):
        x = x_s[...]
        h = rms_normed(x).astype(BF16)
        with jax.named_scope(f"await0_{l}"):
            for k in range(3 if l == 0 else 7):
                attn_copy(l, k).wait()
        if l == 0:
            start_up(0, 0)
        qc = 256
        for c in range(heads * hd // qc):
            qq = jnp.dot(h, wq_s[:, c * qc:(c + 1) * qc], preferred_element_type=F32)
            for s in range(qc // hd):
                hh = c * (qc // hd) + s
                q_s[hh * tok:(hh + 1) * tok, :] = rotary(qq[:, s * hd:(s + 1) * hd]).astype(BF16).astype(F32)
        kk = jnp.dot(h, wk_s[...], preferred_element_type=F32)
        k_new = [rotary(kk[:, s * hd:(s + 1) * hd]).astype(BF16).astype(F32) for s in range(kvh)]
        vv = jnp.dot(h, wv_s[...], preferred_element_type=F32).astype(BF16).astype(F32)
        v_new = [vv[:, s * hd:(s + 1) * hd] for s in range(kvh)]
        if l == 0:
            with jax.named_scope(f"await3_{l}"):
                attn_copy(l, 3).wait()
                attn_copy(l, 4).wait()
            start_up(0, 1)
        for t in range(tok):
            qt = q_s[pl.ds(t, heads, stride=tok), :].astype(BF16)
            st = lax.dot_general(qt, kb[t], NT, preferred_element_type=F32) * scale
            for b in range(kvh * seq // 128):
                s_s[b, pl.ds(t, heads, stride=tok), :] = st[:, b * 128:(b + 1) * 128]
        lane = lax.broadcasted_iota(jnp.int32, (tok, 128), 1)
        w_new = []
        den = []
        for hh in range(heads):
            kv = hh // group
            sl = slice(hh * tok, (hh + 1) * tok)
            sn = jnp.sum(q_s[sl, :] * k_new[kv], axis=-1, keepdims=True) * scale
            blocks = []
            for b in range(kvh * seq // 128):
                col = lane + b * 128
                ok = (lax.rem(col, kvh) == kv) & (col // kvh < len_i)
                blocks.append(jnp.where(ok, s_s[b, sl, :], -jnp.inf))
            top = functools.reduce(jnp.maximum, blocks)
            peak = jnp.maximum(jnp.max(top, axis=-1, keepdims=True), sn)
            ws = [jnp.exp(v - peak) for v in blocks]
            for b, w in enumerate(ws):
                s_s[b, sl, :] = w
            wn = jnp.exp(sn - peak)
            w_new.append(wn)
            den.append(jnp.sum(functools.reduce(jnp.add, ws), axis=-1, keepdims=True) + wn)
        for t in range(tok):
            pt = jnp.concatenate(
                [s_s[b, pl.ds(t, heads, stride=tok), :] for b in range(kvh * seq // 128)], axis=1).astype(BF16)
            o_s[pl.ds(t, heads, stride=tok), :] = jnp.dot(pt, vb[t], preferred_element_type=F32)
        pieces = []
        for hh in range(heads):
            sl = slice(hh * tok, (hh + 1) * tok)
            mixed = o_s[sl, :] + w_new[hh].astype(BF16).astype(F32) * v_new[hh // group]
            pieces.append((mixed / den[hh]).astype(BF16))
        o = jnp.concatenate(pieces, axis=1)
        if l == 0:
            with jax.named_scope(f"await5_{l}"):
                attn_copy(l, 5).wait()
            start_up(0, 2)
        oc = 256
        for c in range(model // oc):
            sl = slice(c * oc, (c + 1) * oc)
            a_s[:, sl] = (x[:, sl] + jnp.dot(o, wo_s[:, sl], preferred_element_type=F32)).astype(BF16).astype(F32)

    def u_copy(l, k):
        view = u_all.at[l, me]
        return pltpu.make_async_remote_copy(
            src_ref=view, dst_ref=view, send_sem=sem_us.at[l], recv_sem=sem_u.at[l, k],
            device_id=peer(*chips[k], 1)[1], device_id_type=MESH)

    def u_relay(l, k):
        view = u_all.at[l, peer(*chips[k], 1)[0]]
        return pltpu.make_async_remote_copy(
            src_ref=view, dst_ref=view, send_sem=sem_us.at[l], recv_sem=sem_u.at[l, 0],
            device_id=peer(0, 0, 1)[1], device_id_type=MESH)

    def u_arrival(l, k):
        view = u_all.at[l, peer(*chips[k], 1)[0]]
        return pltpu.make_async_copy(view, view, sem_u.at[l, k])

    def g_copy(l, j):
        view = g_all.at[l, me]
        return pltpu.make_async_remote_copy(
            src_ref=view, dst_ref=view, send_sem=sem_gs.at[l], recv_sem=sem_g.at[l],
            device_id=peer(*others[j])[1], device_id_type=MESH)

    def wait_all(view, sem):
        pltpu.make_async_copy(view, view, sem).wait()

    def d_copy(l, n, k):
        dest = peer(0, 0, 1)[0] if k == 0 else peer(*chips[k], 0)[0]
        return pltpu.make_async_remote_copy(
            src_ref=part.at[l, n, dest], dst_ref=sbuf.at[l, n, k], send_sem=sem_ds.at[l], recv_sem=sem_d.at[l, n],
            device_id=peer(0, 0, 1)[1], device_id_type=MESH)

    def c_copy(l, n, k):
        return pltpu.make_async_remote_copy(
            src_ref=red.at[l, n, k], dst_ref=rbuf.at[l, n, k], send_sem=sem_cs.at[l], recv_sem=sem_c.at[l, n],
            device_id=peer(*chips[k], 1)[1], device_id_type=MESH)

    far_first = (3, 1, 2)

    def route(l):
        u = rms_normed(a_s[...]).astype(BF16)
        u_all[l, me] = u
        for k in far_first + (0,):
            u_copy(l, k).start()
        if l == 0:
            with jax.named_scope(f"await6_{l}"):
                attn_copy(l, 6).wait()
        rest = wr_s[...]
        n_exp = rest.shape[0]
        logits = jnp.zeros((tok, n_exp), F32)
        for _ in range(3):
            piece = rest.astype(BF16)
            rest = rest - piece.astype(F32)
            logits = logits + lax.dot_general(u, piece, NT, preferred_element_type=F32)
        mine = idt_s[l, pl.ds(row0, tok), :]
        expert = lax.broadcasted_iota(jnp.int32, (tok, n_exp), 1).astype(F32)
        chosen = jnp.zeros((tok, n_exp), jnp.bool_)
        for k in range(mine.shape[1]):
            chosen = chosen | (mine[:, k:k + 1] == expert)
        masked = jnp.where(chosen, logits, -jnp.inf)
        w = jnp.exp(masked - jnp.max(masked, axis=-1, keepdims=True))
        gates = w / jnp.sum(w, axis=-1, keepdims=True)
        g_all[l, me] = jnp.concatenate([gates, jnp.zeros((tok, 128 - n_exp), F32)], axis=1)
        for j in range(len(others)):
            g_copy(l, j).start()

    n_tok = n_dev * tok
    fc = 256

    def up_block(l, lo, hi):
        for i in range(lo, hi):
            ub = u_all[l].reshape(n_tok, model)
            for n in range(ff // fc):
                sl = slice(n * fc, (n + 1) * fc)
                one = jnp.dot(ub, w1_s[i, :, sl], preferred_element_type=F32)
                three = jnp.dot(ub, w3_s[i, :, sl], preferred_element_type=F32)
                inner_s[i, :, sl] = (jax.nn.silu(one) * three).astype(BF16)

    def gate_columns(l):
        gates = g_all[l].reshape(n_tok, 128)
        lane = lax.broadcasted_iota(jnp.int32, (n_tok, 128), 1)
        first = (ep * n_pool + p) * n_loc
        for i in range(n_loc):
            g = jnp.sum(jnp.where(lane == first + i, gates, 0.0), axis=-1, keepdims=True)
            gb_s[i] = jnp.broadcast_to(g, (n_tok, 128))

    def down_block(l, n):
        acc = [jnp.zeros((n_tok, 128), F32) for _ in range(cw // 128)]
        for i in range(n_loc):
            y = jnp.dot(inner_s[i], w2_s[n, i], preferred_element_type=F32).astype(BF16).astype(F32)
            g = gb_s[i]
            for b in range(cw // 128):
                acc[b] = acc[b] + jnp.where(g > 0.0, g * y[:, b * 128:(b + 1) * 128], 0.0)
        for b in range(cw // 128):
            part[l, n, :, :, b * 128:(b + 1) * 128] = acc[b].reshape(n_dev, tok, 128)

    def forward_chunk(l, n):
        wait_all(sbuf.at[l, n], sem_d.at[l, n])
        for k in far_first:
            red[l, n, k] = part[l, n, peer(*chips[k], 1)[0]] + sbuf[l, n, k]
            c_copy(l, n, k).start()

    def up_wait(l, g):
        with jax.named_scope(f"upwait{l}"):
            for c in up_copies(l, g):
                c.wait()

    def experts(l):
        with jax.named_scope(f"uwait{l}"):
            for k in (2, 3, 1):
                u_arrival(l, k).wait()
                u_relay(l, k).start()
        with jax.named_scope(f"urelay{l}"):
            wait_all(u_all.at[l, pl.ds(0, 4)], sem_u.at[l, 0])
        n_pair = n_loc // 2
        step = 1 if l == 0 else 2
        if l > 0:
            down_copy(l, 0).start()
            down_copy(l, 1).start()
        for g in range(0, n_pair, step):
            for s in range(step):
                up_wait(l, g + s)
            if l == 0 and g > 0:
                down_copy(l, g - 1).start()
            if l > 0 and g > 0:
                down_copy(l, 2).start()
                down_copy(l, 3).start()
            with jax.named_scope(f"up{l}"):
                up_block(l, g * 2, (g + step) * 2)
            if g == 0:
                with jax.named_scope(f"gwait{l}"):
                    wait_all(g_all.at[l, pl.ds(0, len(others))], sem_g.at[l])
                gate_columns(l)
        if l == 0:
            down_copy(l, n_chunk - 1).start()
        for n in range(n_chunk):
            with jax.named_scope(f"downwait{l}"):
                down_copy(l, n).wait()
            if l + 1 < layers:
                if n == 0:
                    for k in range(7):
                        attn_copy(l + 1, k).start()
                else:
                    start_up(l + 1, n - 1)
            with jax.named_scope(f"down{l}"):
                down_block(l, n)
            for k in far_first + (0,):
                d_copy(l, n, k).start()
            if n > 0:
                with jax.named_scope(f"fwd{l}"):
                    forward_chunk(l, n - 1)
        if l + 1 < layers:
            start_up(l + 1, n_pair - 1)
        with jax.named_scope(f"fwd{l}"):
            forward_chunk(l, n_chunk - 1)

    other = 1 - p
    orow = pl.multiple_of(other * tok, tok)

    def x_copy(n, row):
        view = xfin.at[pl.ds(row, tok), pl.ds(n * cw, cw)]
        return pltpu.make_async_remote_copy(
            src_ref=view, dst_ref=view, send_sem=sem_x.at[0], recv_sem=sem_x.at[1],
            device_id={"pool": other, "ep": ep}, device_id_type=MESH)

    def combine(l):
        for n in range(n_chunk):
            total = part[l, n, me] + sbuf[l, n, 0]
            wait_all(rbuf.at[l, n, pl.ds(1, 3)], sem_c.at[l, n])
            for k in far_first:
                total = total + rbuf[l, n, k]
            sl = slice(n * cw, (n + 1) * cw)
            x = (a_s[:, sl] + total).astype(BF16)
            if l + 1 < layers:
                x_s[:, sl] = x.astype(F32)
            else:
                xfin[pl.ds(row0, tok), sl] = x
                x_copy(n, row0).start()

    for l in range(layers):
        with jax.named_scope(f"attention{l}"):
            attention(l)
        if l == 0:
            with jax.named_scope("barrier"):
                pl.semaphore_wait(barrier, len(others))
        with jax.named_scope(f"route{l}"):
            route(l)
        if l == 0:
            start_up(0, 3)
        experts(l)
        with jax.named_scope(f"combine{l}"):
            combine(l)

    with jax.named_scope("xwait"):
        wait_all(xfin.at[pl.ds(orow, tok)], sem_x.at[1])
    with jax.named_scope("drain"):
        wait_all(xfin.at[pl.ds(row0, tok)], sem_x.at[0])
        for l in range(layers):
            wait_all(u_all.at[l, pl.ds(0, 7)], sem_us.at[l])
            wait_all(g_all.at[l, pl.ds(0, 7)], sem_gs.at[l])
            wait_all(part.at[l, pl.ds(0, n_chunk // 2)], sem_ds.at[l])
            wait_all(red.at[l, :, pl.ds(1, 3)], sem_cs.at[l])


def solution(mesh):
    n_pool = mesh.shape["pool"]
    n_ep = mesh.shape["ep"]
    n_dev = n_pool * n_ep

    def body(hidden, k_cache, v_cache, lengths, expert_ids, w_query, w_key, w_value, w_out, w_router, w_gate, w_up, w_down):
        layers, n_tok, seq, kvh, hd = k_cache.shape
        tok = n_tok // n_pool
        model = hidden.shape[1]
        heads = w_query.shape[2] // hd
        n_loc = w_gate.shape[1] // n_pool
        ff = w_gate.shape[3]
        n_exp = w_router.shape[2]
        topk = expert_ids.shape[2]
        cw = 256
        n_chunk = model // cw
        kflat = k_cache.reshape(layers, n_tok, seq * kvh, hd)
        vflat = v_cache.reshape(layers, n_tok, seq * kvh, hd)
        ids = jnp.swapaxes(expert_ids, 1, 2)
        router = jnp.swapaxes(w_router, 1, 2)
        cfg = (layers, n_pool, n_ep, tok, heads, kvh, hd, seq, n_loc, ff, model)
        any_spec = pl.BlockSpec(memory_space=pl.ANY)
        vm = pltpu.VMEM
        dma = pltpu.SemaphoreType.DMA
        return pl.pallas_call(
            functools.partial(kernel, cfg),
            out_shape=vm((n_tok, model), BF16),
            in_specs=[any_spec] * 13,
            out_specs=pl.BlockSpec(memory_space=pltpu.VMEM),
            scratch_shapes=[
                vm((model, heads * hd), BF16), vm((model, kvh * hd), BF16), vm((model, kvh * hd), BF16),
                vm((heads * hd, model), BF16), vm((n_exp, model), F32),
                vm((tok, seq * kvh, hd), BF16), vm((tok, seq * kvh, hd), BF16),
                vm((n_loc, model, ff), BF16), vm((n_loc, model, ff), BF16), vm((n_chunk, n_loc, ff, cw), BF16),
                vm((tok, model), F32), vm((tok, model), F32), vm((layers, topk, n_tok), jnp.int32), vm((layers, 128, topk), F32),
                vm((heads * tok, hd), F32), vm((kvh * seq // 128, heads * tok, 128), F32), vm((heads * tok, hd), F32),
                vm((layers, n_dev, tok, model), BF16), vm((layers, n_dev, tok, 128), F32), vm((n_loc, n_dev * tok, 128), F32),
                vm((n_loc, n_dev * tok, ff), BF16), vm((layers, n_chunk, n_dev, tok, cw), F32),
                vm((layers, n_chunk, 4, tok, cw), F32), vm((layers, n_chunk, 4, tok, cw), F32), vm((layers, n_chunk, 4, tok, cw), F32),
                vm((tok, model), BF16), pltpu.SMEM((n_tok,), jnp.int32),
                dma((10,)), dma((2, n_loc // 2)), dma((n_chunk,)), dma((layers, 4)), dma((layers,)), dma((layers,)), dma((layers,)),
                dma((layers, n_chunk)), dma((layers,)), dma((layers, n_chunk)), dma((layers,)), dma((2,)),
            ],
            compiler_params=pltpu.CompilerParams(
                collective_id=0, has_side_effects=True, vmem_limit_bytes=63 * 1024 * 1024),
        )(hidden, kflat, vflat, lengths, ids, w_query, w_key, w_value, w_out, router, w_gate, w_up, w_down)

    rows_spec = ("dp", "ep")
    in_specs = (P(rows_spec, None), P(None, rows_spec), P(None, rows_spec), P(rows_spec), P(None, rows_spec, None), P(), P(), P(), P(), P(), P(None, "ep"), P(None, "ep"), P(None, "ep"))
    return jax.shard_map(body, mesh=mesh, in_specs=in_specs, out_specs=P(rows_spec, None), check_vma=False)
```

```python
import functools
import math

import jax
import jax.numpy as jnp
from jax import lax
from jax.experimental import pallas as pl
from jax.experimental.pallas import tpu as pltpu
from jax.sharding import PartitionSpec as P

EPSILON = 1e-6
ROPE_BASE = 10000.0
MESH = pl.DeviceIdType.MESH
F32 = jnp.float32
BF16 = jnp.bfloat16
NT = (((1,), (1,)), ((), ()))


def rms_normed(values):
    return values * lax.rsqrt(jnp.mean(values * values, axis=-1, keepdims=True) + EPSILON)


def kernel(cfg, hid, kc, vc, lens, ids, wq, wk, wv, wo, wr, wg, wu, wd, xfin,
           wq_s, wk_s, wv_s, wo_s, wr_s, kb, vb, w1_s, w3_s, w2_s,
           x_s, a_s, ids_s, idt_s, q_s, s_s, o_s,
           u_all, g_all, gb_s, inner_s, part, sbuf, red, rbuf, sbuf2, red2, rbuf2, abuf, hid_s, lens_s,
           sem_a, sem_w, sem_w2, sem_u, sem_us, sem_g, sem_gs, sem_d, sem_ds, sem_c, sem_cs, sem_x):
    layers, n_pool, n_ep, tok, heads, kvh, hd, seq, n_loc, ff, model = cfg
    n_dev = n_pool * n_ep
    n_chunk, _, _, cw = w2_s.shape
    n_both = sbuf2.shape[0]
    p = lax.axis_index("pool")
    ep = lax.axis_index("ep")
    me = p * n_ep + ep
    row0 = pl.multiple_of(p * tok, tok)

    cx = ep // 2
    cc = lax.rem(ep, 2)

    def peer(dy, dx, dc):
        y, e = lax.rem(p + dy, 2), lax.rem(cx + dx, 2) * 2 + lax.rem(cc + dc, 2)
        return y * n_ep + e, {"pool": y, "ep": e}

    others = [(1, 1, 1), (1, 1, 0), (0, 1, 1), (1, 0, 1), (0, 1, 0), (1, 0, 0), (0, 0, 1)]
    chips = [(0, 0), (0, 1), (1, 0), (1, 1)]

    def attn_copy(l, k):
        src, dst = [
            (lambda: wq.at[l], wq_s), (lambda: wk.at[l], wk_s), (lambda: wv.at[l], wv_s),
            (lambda: kc.at[l, pl.ds(row0, tok)], kb), (lambda: vc.at[l, pl.ds(row0, tok)], vb),
            (lambda: wo.at[l], wo_s), (lambda: wr.at[l], wr_s),
        ][k]
        return pltpu.make_async_copy(src(), dst, sem_a.at[k])

    def up_copies(l, g):
        e = p * n_loc + g * 2
        return [
            pltpu.make_async_copy(wg.at[l, pl.ds(e, 2)], w1_s.at[pl.ds(g * 2, 2)], sem_w.at[0, g]),
            pltpu.make_async_copy(wu.at[l, pl.ds(e, 2)], w3_s.at[pl.ds(g * 2, 2)], sem_w.at[1, g]),
        ]

    def start_up(l, g):
        for c in up_copies(l, g):
            c.start()

    def down_copy(l, n):
        return pltpu.make_async_copy(
            wd.at[l, pl.ds(p * n_loc, n_loc), :, pl.ds(n * cw, cw)], w2_s.at[n], sem_w2.at[n])

    hid_copy = pltpu.make_async_copy(hid.at[pl.ds(row0, tok)], hid_s, sem_a.at[7])
    ids_copy = pltpu.make_async_copy(ids, ids_s, sem_a.at[8])
    len_copy = pltpu.make_async_copy(lens, lens_s, sem_a.at[9])
    len_copy.start()
    hid_copy.start()
    ids_copy.start()
    for k in range(3):
        attn_copy(0, k).start()

    barrier = pltpu.get_barrier_semaphore()
    for rel in others:
        pl.semaphore_signal(barrier, inc=1, device_id=peer(*rel)[1], device_id_type=MESH)

    with jax.named_scope("lenwait"):
        len_copy.wait()
    rows = lax.broadcasted_iota(jnp.int32, (tok, hd), 0)
    lanes = lax.broadcasted_iota(jnp.int32, (tok, hd), 1)
    len_i = jnp.zeros((tok, hd), jnp.int32)
    for t in range(tok):
        len_i = jnp.where(rows == t, lens_s[p * tok + t], len_i)
    half = hd // 2
    pair = jnp.where(lanes < half, lanes, lanes - half).astype(F32)
    freq = jnp.exp(pair * (-2.0 * math.log(ROPE_BASE) / hd))
    angle = len_i.astype(F32) * freq
    cosine = jnp.cos(angle)
    sine = jnp.sin(angle)
    sine = jnp.where(lanes < half, -sine, sine)

    def rotary(v):
        return v * cosine + pltpu.roll(v, half, 1) * sine

    with jax.named_scope("idswait"):
        ids_copy.wait()
    for l in range(layers):
        idf = jnp.concatenate([ids_s[l].astype(F32), jnp.zeros((ids_s.shape[1], 128 - ids_s.shape[2]), F32)], axis=1)
        idt_s[l] = jnp.transpose(idf)
    for k in range(3, 7):
        attn_copy(0, k).start()
    with jax.named_scope("hidwait"):
        hid_copy.wait()
    x_s[...] = hid_s[...].astype(F32)

    scale = hd ** -0.5
    group = heads // kvh

    def attention(l):
        x = x_s[...]
        h = rms_normed(x).astype(BF16)
        with jax.named_scope(f"await0_{l}"):
            for k in range(3 if l == 0 else 7):
                attn_copy(l, k).wait()
        qc = 256
        for c in range(heads * hd // qc):
            qq = jnp.dot(h, wq_s[:, c * qc:(c + 1) * qc], preferred_element_type=F32)
            for s in range(qc // hd):
                hh = c * (qc // hd) + s
                q_s[hh * tok:(hh + 1) * tok, :] = rotary(qq[:, s * hd:(s + 1) * hd]).astype(BF16).astype(F32)
        kk = jnp.dot(h, wk_s[...], preferred_element_type=F32)
        k_new = [rotary(kk[:, s * hd:(s + 1) * hd]).astype(BF16).astype(F32) for s in range(kvh)]
        vv = jnp.dot(h, wv_s[...], preferred_element_type=F32).astype(BF16).astype(F32)
        v_new = [vv[:, s * hd:(s + 1) * hd] for s in range(kvh)]
        if l == 0:
            with jax.named_scope(f"await3_{l}"):
                attn_copy(l, 3).wait()
                attn_copy(l, 4).wait()
            start_up(0, 0)
        for t in range(tok):
            qt = q_s[pl.ds(t, heads, stride=tok), :].astype(BF16)
            st = lax.dot_general(qt, kb[t], NT, preferred_element_type=F32) * scale
            for b in range(kvh * seq // 128):
                s_s[b, pl.ds(t, heads, stride=tok), :] = st[:, b * 128:(b + 1) * 128]
        lane = lax.broadcasted_iota(jnp.int32, (tok, 128), 1)
        w_new = []
        den = []
        for hh in range(heads):
            kv = hh // group
            sl = slice(hh * tok, (hh + 1) * tok)
            sn = jnp.sum(q_s[sl, :] * k_new[kv], axis=-1, keepdims=True) * scale
            blocks = []
            for b in range(kvh * seq // 128):
                col = lane + b * 128
                ok = (lax.rem(col, kvh) == kv) & (col // kvh < len_i)
                blocks.append(jnp.where(ok, s_s[b, sl, :], -jnp.inf))
            top = functools.reduce(jnp.maximum, blocks)
            peak = jnp.maximum(jnp.max(top, axis=-1, keepdims=True), sn)
            ws = [jnp.exp(v - peak) for v in blocks]
            for b, w in enumerate(ws):
                s_s[b, sl, :] = w
            wn = jnp.exp(sn - peak)
            w_new.append(wn)
            den.append(jnp.sum(functools.reduce(jnp.add, ws), axis=-1, keepdims=True) + wn)
        for t in range(tok):
            pt = jnp.concatenate(
                [s_s[b, pl.ds(t, heads, stride=tok), :] for b in range(kvh * seq // 128)], axis=1).astype(BF16)
            o_s[pl.ds(t, heads, stride=tok), :] = jnp.dot(pt, vb[t], preferred_element_type=F32)
        pieces = []
        for hh in range(heads):
            sl = slice(hh * tok, (hh + 1) * tok)
            mixed = o_s[sl, :] + w_new[hh].astype(BF16).astype(F32) * v_new[hh // group]
            pieces.append((mixed / den[hh]).astype(BF16))
        o = jnp.concatenate(pieces, axis=1)
        if l == 0:
            with jax.named_scope(f"await5_{l}"):
                attn_copy(l, 5).wait()
            start_up(0, 1)
            start_up(0, 2)
        oc = 256
        for c in range(model // oc):
            sl = slice(c * oc, (c + 1) * oc)
            a_s[:, sl] = (x[:, sl] + jnp.dot(o, wo_s[:, sl], preferred_element_type=F32)).astype(BF16).astype(F32)

    def u_copy(l, k):
        view = u_all.at[l, me]
        return pltpu.make_async_remote_copy(
            src_ref=view, dst_ref=view, send_sem=sem_us.at[0], recv_sem=sem_u.at[k],
            device_id=peer(*chips[k], 1)[1], device_id_type=MESH)

    def u_relay(l, k):
        view = u_all.at[l, peer(*chips[k], 1)[0]]
        return pltpu.make_async_remote_copy(
            src_ref=view, dst_ref=view, send_sem=sem_us.at[0], recv_sem=sem_u.at[0],
            device_id=peer(0, 0, 1)[1], device_id_type=MESH)

    def u_arrival(l, k):
        view = u_all.at[l, peer(*chips[k], 1)[0]]
        return pltpu.make_async_copy(view, view, sem_u.at[k])

    def g_copy(l, j):
        view = g_all.at[l, me]
        return pltpu.make_async_remote_copy(
            src_ref=view, dst_ref=view, send_sem=sem_gs.at[0], recv_sem=sem_g.at[0],
            device_id=peer(*others[j])[1], device_id_type=MESH)

    def wait_all(view, sem):
        pltpu.make_async_copy(view, view, sem).wait()

    def d_copy(l, n, k):
        dest = peer(0, 0, 1)[0] if k == 0 else peer(*chips[k], 0)[0]
        return pltpu.make_async_remote_copy(
            src_ref=part.at[l, n, dest], dst_ref=sbuf.at[l, n, k], send_sem=sem_ds.at[0], recv_sem=sem_d.at[n],
            device_id=peer(0, 0, 1)[1], device_id_type=MESH)

    def c_copy(l, n, k):
        return pltpu.make_async_remote_copy(
            src_ref=red.at[l, n, k], dst_ref=rbuf.at[l, n, k], send_sem=sem_cs.at[0], recv_sem=sem_c.at[n],
            device_id=peer(*chips[k], 1)[1], device_id_type=MESH)

    far_first = (3, 1, 2)

    def route(l):
        u = rms_normed(a_s[...]).astype(BF16)
        u_all[l, me] = u
        for k in far_first + (0,):
            u_copy(l, k).start()
        if l == 0:
            with jax.named_scope(f"await6_{l}"):
                attn_copy(l, 6).wait()
        rest = wr_s[...]
        n_exp = rest.shape[0]
        logits = jnp.zeros((tok, n_exp), F32)
        for _ in range(3):
            piece = rest.astype(BF16)
            rest = rest - piece.astype(F32)
            logits = logits + lax.dot_general(u, piece, NT, preferred_element_type=F32)
        mine = idt_s[l, pl.ds(row0, tok), :]
        expert = lax.broadcasted_iota(jnp.int32, (tok, n_exp), 1).astype(F32)
        chosen = jnp.zeros((tok, n_exp), jnp.bool_)
        for k in range(mine.shape[1]):
            chosen = chosen | (mine[:, k:k + 1] == expert)
        masked = jnp.where(chosen, logits, -jnp.inf)
        w = jnp.exp(masked - jnp.max(masked, axis=-1, keepdims=True))
        gates = w / jnp.sum(w, axis=-1, keepdims=True)
        g_all[l, me] = jnp.concatenate([gates, jnp.zeros((tok, 128 - n_exp), F32)], axis=1)
        for j in range(len(others)):
            g_copy(l, j).start()

    n_tok = n_dev * tok
    fc = 256

    def up_block(l, lo, hi):
        for i in range(lo, hi):
            ub = u_all[l].reshape(n_tok, model)
            for n in range(ff // fc):
                sl = slice(n * fc, (n + 1) * fc)
                one = jnp.dot(ub, w1_s[i, :, sl], preferred_element_type=F32)
                three = jnp.dot(ub, w3_s[i, :, sl], preferred_element_type=F32)
                inner_s[i, :, sl] = (jax.nn.silu(one) * three).astype(BF16)

    def gate_columns(l):
        gates = g_all[l].reshape(n_tok, 128)
        first = (ep * n_pool + p) * n_loc
        gates = pltpu.roll(gates, lax.rem(128 - first, 128), 1)
        for i in range(n_loc):
            gb_s[i] = jnp.broadcast_to(gates[:, i:i + 1], (n_tok, 128))

    def down_block(l, n):
        acc = [jnp.zeros((n_tok, 128), F32) for _ in range(cw // 128)]
        for i in range(n_loc):
            y = jnp.dot(inner_s[i], w2_s[n, i], preferred_element_type=F32).astype(BF16).astype(F32)
            g = gb_s[i]
            for b in range(cw // 128):
                acc[b] = acc[b] + jnp.where(g > 0.0, g * y[:, b * 128:(b + 1) * 128], 0.0)
        for b in range(cw // 128):
            part[l, n, :, :, b * 128:(b + 1) * 128] = acc[b].reshape(n_dev, tok, 128)

    def both(l, n):
        return l == layers - 1 and n >= n_chunk - n_both

    def d2_copy(l, n, k):
        dest = peer(*chips[k], 0)[0] if k < 4 else peer(*chips[(k - 4) * 2], 1)[0]
        return pltpu.make_async_remote_copy(
            src_ref=part.at[l, n, dest], dst_ref=sbuf2.at[n - n_chunk + n_both, k], send_sem=sem_ds.at[1], recv_sem=sem_d.at[n],
            device_id=peer(0, 0, 1)[1], device_id_type=MESH)

    def c2_copy(n, k, r):
        m = n - n_chunk + n_both
        return pltpu.make_async_remote_copy(
            src_ref=red2.at[m, (k + 2 * r) % 4], dst_ref=rbuf2.at[m, k, r], send_sem=sem_cs.at[1], recv_sem=sem_c.at[n],
            device_id=peer(*chips[k], 1)[1], device_id_type=MESH)

    def share_chunk(l, n):
        if both(l, n):
            for k in (3, 1, 2, 0, 4, 5):
                d2_copy(l, n, k).start()
        else:
            for k in far_first + (0,):
                d_copy(l, n, k).start()

    def forward_chunk(l, n):
        if both(l, n):
            m = n - n_chunk + n_both
            wait_all(sbuf2.at[m], sem_d.at[n])
            for k in (3, 1, 2, 0):
                red2[m, k] = part[l, n, peer(*chips[k], 1)[0]] + sbuf2[m, k]
                if k == 1:
                    for q in (3, 1):
                        for r in range(2):
                            c2_copy(n, q, r).start()
            for r in range(2):
                c2_copy(n, 2, r).start()
            return
        wait_all(sbuf.at[l, n], sem_d.at[n])
        for k in far_first:
            red[l, n, k] = part[l, n, peer(*chips[k], 1)[0]] + sbuf[l, n, k]
            c_copy(l, n, k).start()

    def up_wait(l, g):
        with jax.named_scope(f"upwait{l}"):
            for c in up_copies(l, g):
                c.wait()

    def experts(l):
        with jax.named_scope(f"uwait{l}"):
            for k in (2, 3, 1):
                u_arrival(l, k).wait()
                u_relay(l, k).start()
        with jax.named_scope(f"urelay{l}"):
            wait_all(u_all.at[l, pl.ds(0, 4)], sem_u.at[0])
        n_pair = n_loc // 2
        if l > 0:
            down_copy(l, 0).start()
            down_copy(l, 1).start()
        blocks = (2, 2) if l == 0 else (4,)
        lo = 0
        for gi, step in enumerate(blocks):
            for g in range(lo, lo + step):
                up_wait(l, g)
            if gi == len(blocks) - 1:
                for n in range(2, n_chunk):
                    down_copy(l, n).start()
            elif l == 0:
                for n in range(2):
                    down_copy(l, n).start()
            if gi == 0:
                wait_all(g_all.at[l, pl.ds(0, len(others))], sem_g.at[0])
            with jax.named_scope(f"up{l}"):
                up_block(l, lo * 2, (lo + step) * 2)
                if gi == 0:
                    gate_columns(l)
            lo += step
        for n in range(n_chunk):
            with jax.named_scope(f"downwait{l}"):
                down_copy(l, n).wait()
            if l + 1 < layers:
                if n == 0:
                    for k in range(7):
                        attn_copy(l + 1, k).start()
                else:
                    start_up(l + 1, n - 1)
            with jax.named_scope(f"down{l}"):
                down_block(l, n)
            share_chunk(l, n)
            if n > 0:
                with jax.named_scope(f"fwd{l}"):
                    forward_chunk(l, n - 1)
        if l + 1 < layers:
            start_up(l + 1, n_pair - 1)
        with jax.named_scope(f"fwd{l}"):
            forward_chunk(l, n_chunk - 1)

    other = 1 - p
    orow = pl.multiple_of(other * tok, tok)

    def x_copy(n, row):
        view = xfin.at[pl.ds(row, tok), pl.ds(n * cw, cw)]
        return pltpu.make_async_remote_copy(
            src_ref=view, dst_ref=view, send_sem=sem_x.at[0], recv_sem=sem_x.at[1],
            device_id={"pool": other, "ep": ep}, device_id_type=MESH)

    def a_copy():
        return pltpu.make_async_remote_copy(
            src_ref=abuf.at[0], dst_ref=abuf.at[1], send_sem=sem_x.at[2], recv_sem=sem_x.at[3],
            device_id={"pool": other, "ep": ep}, device_id_type=MESH)

    def combine(l):
        for n in range(n_chunk):
            sl = slice(n * cw, (n + 1) * cw)
            if both(l, n):
                m = n - n_chunk + n_both
                if m == 0:
                    a_copy().wait_recv()
                wait_all(rbuf2.at[m, pl.ds(1, 3)], sem_c.at[n])
                ac = slice(m * cw, (m + 1) * cw)
                for r in range(2):
                    total = part[l, n, peer(*chips[2 * r], 0)[0]] + sbuf2[m, 4 + r]
                    total = (total + rbuf2[m, 2, r]) + (rbuf2[m, 1, r] + rbuf2[m, 3, r])
                    xfin[pl.ds(orow if r else row0, tok), sl] = (abuf[r, :, ac].astype(F32) + total).astype(BF16)
                continue
            total = part[l, n, me] + sbuf[l, n, 0]
            wait_all(rbuf.at[l, n, pl.ds(1, 3)], sem_c.at[n])
            total = (total + rbuf[l, n, 2]) + (rbuf[l, n, 1] + rbuf[l, n, 3])
            x = (a_s[:, sl] + total).astype(BF16)
            if l + 1 < layers:
                x_s[:, sl] = x.astype(F32)
            else:
                xfin[pl.ds(row0, tok), sl] = x
                x_copy(n, row0).start()

    for l in range(layers):
        with jax.named_scope(f"attention{l}"):
            attention(l)
        if l == 0:
            with jax.named_scope("barrier"):
                pl.semaphore_wait(barrier, len(others))
        with jax.named_scope(f"route{l}"):
            route(l)
        if l == 0:
            start_up(0, 3)
        if l == layers - 1:
            abuf[0] = a_s[:, model - n_both * cw:].astype(BF16)
            a_copy().start()
        experts(l)
        with jax.named_scope(f"combine{l}"):
            combine(l)

    with jax.named_scope("xwait"):
        wait_all(xfin.at[pl.ds(orow, tok), pl.ds(0, model - n_both * cw)], sem_x.at[1])
    with jax.named_scope("drain"):
        wait_all(xfin.at[pl.ds(row0, tok), pl.ds(0, model - n_both * cw)], sem_x.at[0])
        a_copy().wait_send()
        wait_all(u_all.at[:, pl.ds(0, 7)], sem_us.at[0])
        wait_all(g_all.at[:, pl.ds(0, 7)], sem_gs.at[0])
        wait_all(part.at[0, pl.ds(0, n_chunk - n_both // 2)], sem_ds.at[0])
        wait_all(part.at[0, pl.ds(0, n_both), pl.ds(0, 6)], sem_ds.at[1])
        wait_all(red.at[:, pl.ds(0, n_chunk - n_both // 2), pl.ds(1, 3)], sem_cs.at[0])
        wait_all(red.at[:, pl.ds(0, n_both), pl.ds(1, 3)], sem_cs.at[1])


def solution(mesh):
    n_pool = mesh.shape["pool"]
    n_ep = mesh.shape["ep"]
    n_dev = n_pool * n_ep

    def body(hidden, k_cache, v_cache, lengths, expert_ids, w_query, w_key, w_value, w_out, w_router, w_gate, w_up, w_down):
        layers, n_tok, seq, kvh, hd = k_cache.shape
        tok = n_tok // n_pool
        model = hidden.shape[1]
        heads = w_query.shape[2] // hd
        n_loc = w_gate.shape[1] // n_pool
        ff = w_gate.shape[3]
        n_exp = w_router.shape[2]
        topk = expert_ids.shape[2]
        cw = 256
        n_chunk = model // cw
        n_both = n_chunk // 2
        kflat = k_cache.reshape(layers, n_tok, seq * kvh, hd)
        vflat = v_cache.reshape(layers, n_tok, seq * kvh, hd)
        ids = jnp.swapaxes(expert_ids, 1, 2)
        router = jnp.swapaxes(w_router, 1, 2)
        cfg = (layers, n_pool, n_ep, tok, heads, kvh, hd, seq, n_loc, ff, model)
        any_spec = pl.BlockSpec(memory_space=pl.ANY)
        vm = pltpu.VMEM
        dma = pltpu.SemaphoreType.DMA
        return pl.pallas_call(
            functools.partial(kernel, cfg),
            out_shape=vm((n_tok, model), BF16),
            in_specs=[any_spec] * 13,
            out_specs=pl.BlockSpec(memory_space=pltpu.VMEM),
            scratch_shapes=[
                vm((model, heads * hd), BF16), vm((model, kvh * hd), BF16), vm((model, kvh * hd), BF16),
                vm((heads * hd, model), BF16), vm((n_exp, model), F32),
                vm((tok, seq * kvh, hd), BF16), vm((tok, seq * kvh, hd), BF16),
                vm((n_loc, model, ff), BF16), vm((n_loc, model, ff), BF16), vm((n_chunk, n_loc, ff, cw), BF16),
                vm((tok, model), F32), vm((tok, model), F32), vm((layers, topk, n_tok), jnp.int32), vm((layers, 128, topk), F32),
                vm((heads * tok, hd), F32), vm((kvh * seq // 128, heads * tok, 128), F32), vm((heads * tok, hd), F32),
                vm((layers, n_dev, tok, model), BF16), vm((layers, n_dev, tok, 128), F32), vm((n_loc, n_dev * tok, 128), F32),
                vm((n_loc, n_dev * tok, ff), BF16), vm((layers, n_chunk, n_dev, tok, cw), F32),
                vm((layers, n_chunk, 4, tok, cw), F32), vm((layers, n_chunk, 4, tok, cw), F32), vm((layers, n_chunk, 4, tok, cw), F32),
                vm((n_both, 6, tok, cw), F32), vm((n_both, 4, tok, cw), F32), vm((n_both, 4, 2, tok, cw), F32),
                vm((2, tok, n_both * cw), BF16), vm((tok, model), BF16), pltpu.SMEM((n_tok,), jnp.int32),
                dma((10,)), dma((2, n_loc // 2)), dma((n_chunk,)), dma((4,)), dma((1,)), dma((1,)), dma((1,)),
                dma((n_chunk,)), dma((2,)), dma((n_chunk,)), dma((2,)), dma((4,)),
            ],
            compiler_params=pltpu.CompilerParams(
                collective_id=0, has_side_effects=True, vmem_limit_bytes=63 * 1024 * 1024),
        )(hidden, kflat, vflat, lengths, ids, w_query, w_key, w_value, w_out, router, w_gate, w_up, w_down)

    rows_spec = ("dp", "ep")
    in_specs = (P(rows_spec, None), P(None, rows_spec), P(None, rows_spec), P(rows_spec), P(None, rows_spec, None), P(), P(), P(), P(), P(), P(None, "ep"), P(None, "ep"), P(None, "ep"))
    return jax.shard_map(body, mesh=mesh, in_specs=in_specs, out_specs=P(rows_spec, None), check_vma=False)
```

```python
import functools
import math

import jax
import jax.numpy as jnp
from jax import lax
from jax.experimental import pallas as pl
from jax.experimental.pallas import tpu as pltpu
from jax.sharding import PartitionSpec as P

EPSILON = 1e-6
ROPE_BASE = 10000.0
MESH = pl.DeviceIdType.MESH
F32 = jnp.float32
BF16 = jnp.bfloat16
NT = (((1,), (1,)), ((), ()))


def rms_normed(values):
    return values * lax.rsqrt(jnp.mean(values * values, axis=-1, keepdims=True) + EPSILON)


def kernel(cfg, hid, kc, vc, lens, ids, wq, wk, wv, wo, wr, wg, wu, wd, xfin,
           wq_s, wk_s, wv_s, wo_s, wr_s, kb, vb, w1_s, w3_s, w2_s,
           x_s, a_s, ids_s, idt_s, q_s, s_s, o_s,
           a_all, u_all, g_all, gb_s, inner_s, part, sbuf, red, rbuf, sbuf2, red2, rbuf2, hid_s, lens_s,
           sem_a, sem_w, sem_w2, sem_u, sem_us, sem_g, sem_gs, sem_d, sem_ds, sem_c, sem_cs, sem_x):
    layers, n_pool, n_ep, tok, heads, kvh, hd, seq, n_loc, ff, model = cfg
    n_dev = n_pool * n_ep
    n_chunk, _, _, cw = w2_s.shape
    n_both = sbuf2.shape[0]
    p = lax.axis_index("pool")
    ep = lax.axis_index("ep")
    me = p * n_ep + ep
    row0 = pl.multiple_of(p * tok, tok)

    cx = ep // 2
    cc = lax.rem(ep, 2)

    def peer(dy, dx, dc):
        y, e = lax.rem(p + dy, 2), lax.rem(cx + dx, 2) * 2 + lax.rem(cc + dc, 2)
        return y * n_ep + e, {"pool": y, "ep": e}

    others = [(1, 1, 1), (1, 1, 0), (0, 1, 1), (1, 0, 1), (0, 1, 0), (1, 0, 0), (0, 0, 1)]
    chips = [(0, 0), (0, 1), (1, 0), (1, 1)]

    def attn_copy(l, k):
        src, dst = [
            (lambda: wq.at[l], wq_s), (lambda: wk.at[l], wk_s), (lambda: wv.at[l], wv_s),
            (lambda: kc.at[l, pl.ds(row0, tok)], kb), (lambda: vc.at[l, pl.ds(row0, tok)], vb),
            (lambda: wo.at[l], wo_s), (lambda: wr.at[l], wr_s),
        ][k]
        return pltpu.make_async_copy(src(), dst, sem_a.at[k])

    def up_copies(l, g):
        e = p * n_loc + g * 2
        return [
            pltpu.make_async_copy(wg.at[l, pl.ds(e, 2)], w1_s.at[pl.ds(g * 2, 2)], sem_w.at[0, g]),
            pltpu.make_async_copy(wu.at[l, pl.ds(e, 2)], w3_s.at[pl.ds(g * 2, 2)], sem_w.at[1, g]),
        ]

    def start_up(l, g):
        for c in up_copies(l, g):
            c.start()

    def down_copy(l, n):
        return pltpu.make_async_copy(
            wd.at[l, pl.ds(p * n_loc, n_loc), :, pl.ds(n * cw, cw)], w2_s.at[n], sem_w2.at[n])

    hid_copy = pltpu.make_async_copy(hid.at[pl.ds(row0, tok)], hid_s, sem_a.at[7])
    ids_copy = pltpu.make_async_copy(ids, ids_s, sem_a.at[8])
    len_copy = pltpu.make_async_copy(lens, lens_s, sem_a.at[9])
    len_copy.start()
    hid_copy.start()
    ids_copy.start()
    for k in range(3):
        attn_copy(0, k).start()

    barrier = pltpu.get_barrier_semaphore()
    for rel in others:
        pl.semaphore_signal(barrier, inc=1, device_id=peer(*rel)[1], device_id_type=MESH)

    with jax.named_scope("lenwait"):
        len_copy.wait()
    rows = lax.broadcasted_iota(jnp.int32, (tok, hd), 0)
    lanes = lax.broadcasted_iota(jnp.int32, (tok, hd), 1)
    len_i = jnp.zeros((tok, hd), jnp.int32)
    for t in range(tok):
        len_i = jnp.where(rows == t, lens_s[p * tok + t], len_i)
    half = hd // 2
    pair = jnp.where(lanes < half, lanes, lanes - half).astype(F32)
    freq = jnp.exp(pair * (-2.0 * math.log(ROPE_BASE) / hd))
    angle = len_i.astype(F32) * freq
    cosine = jnp.cos(angle)
    sine = jnp.sin(angle)
    sine = jnp.where(lanes < half, -sine, sine)

    def rotary(v):
        return v * cosine + pltpu.roll(v, half, 1) * sine

    with jax.named_scope("idswait"):
        ids_copy.wait()
    for l in range(layers):
        idf = jnp.concatenate([ids_s[l].astype(F32), jnp.zeros((ids_s.shape[1], 128 - ids_s.shape[2]), F32)], axis=1)
        idt_s[l] = jnp.transpose(idf)
    for k in range(3, 7):
        attn_copy(0, k).start()
    with jax.named_scope("hidwait"):
        hid_copy.wait()
    x_s[...] = hid_s[...].astype(F32)

    hw = a_all.shape[4]

    def a_copy(l, h, k):
        view = a_all.at[l, h, me]
        return pltpu.make_async_remote_copy(
            src_ref=view, dst_ref=view, send_sem=sem_us.at[0], recv_sem=sem_u.at[2 * k + h if k else 0],
            device_id=peer(*chips[k], 1)[1], device_id_type=MESH)

    def a_relay(l, h, k):
        view = a_all.at[l, h, peer(*chips[k], 1)[0]]
        return pltpu.make_async_remote_copy(
            src_ref=view, dst_ref=view, send_sem=sem_us.at[0], recv_sem=sem_u.at[0],
            device_id=peer(0, 0, 1)[1], device_id_type=MESH)

    def a_arrival(l, h, k):
        view = a_all.at[l, h, peer(*chips[k], 1)[0]]
        return pltpu.make_async_copy(view, view, sem_u.at[2 * k + h])

    far_first = (3, 1, 2)

    scale = hd ** -0.5
    group = heads // kvh

    def attention(l):
        x = x_s[...]
        h = rms_normed(x).astype(BF16)
        with jax.named_scope(f"await0_{l}"):
            for k in range(3 if l == 0 else 7):
                attn_copy(l, k).wait()
        qc = 256
        for c in range(heads * hd // qc):
            qq = jnp.dot(h, wq_s[:, c * qc:(c + 1) * qc], preferred_element_type=F32)
            for s in range(qc // hd):
                hh = c * (qc // hd) + s
                q_s[hh * tok:(hh + 1) * tok, :] = rotary(qq[:, s * hd:(s + 1) * hd]).astype(BF16).astype(F32)
        kk = jnp.dot(h, wk_s[...], preferred_element_type=F32)
        k_new = [rotary(kk[:, s * hd:(s + 1) * hd]).astype(BF16).astype(F32) for s in range(kvh)]
        vv = jnp.dot(h, wv_s[...], preferred_element_type=F32).astype(BF16).astype(F32)
        v_new = [vv[:, s * hd:(s + 1) * hd] for s in range(kvh)]
        if l == 0:
            with jax.named_scope(f"await3_{l}"):
                attn_copy(l, 3).wait()
                attn_copy(l, 4).wait()
            start_up(0, 0)
        for t in range(tok):
            qt = q_s[pl.ds(t, heads, stride=tok), :].astype(BF16)
            st = lax.dot_general(qt, kb[t], NT, preferred_element_type=F32) * scale
            for b in range(kvh * seq // 128):
                s_s[b, pl.ds(t, heads, stride=tok), :] = st[:, b * 128:(b + 1) * 128]
        lane = lax.broadcasted_iota(jnp.int32, (tok, 128), 1)
        w_new = []
        den = []
        for hh in range(heads):
            kv = hh // group
            sl = slice(hh * tok, (hh + 1) * tok)
            sn = jnp.sum(q_s[sl, :] * k_new[kv], axis=-1, keepdims=True) * scale
            blocks = []
            for b in range(kvh * seq // 128):
                col = lane + b * 128
                ok = (lax.rem(col, kvh) == kv) & (col // kvh < len_i)
                blocks.append(jnp.where(ok, s_s[b, sl, :], -jnp.inf))
            top = functools.reduce(jnp.maximum, blocks)
            peak = jnp.maximum(jnp.max(top, axis=-1, keepdims=True), sn)
            ws = [jnp.exp(v - peak) for v in blocks]
            for b, w in enumerate(ws):
                s_s[b, sl, :] = w
            wn = jnp.exp(sn - peak)
            w_new.append(wn)
            den.append(jnp.sum(functools.reduce(jnp.add, ws), axis=-1, keepdims=True) + wn)
        for t in range(tok):
            pt = jnp.concatenate(
                [s_s[b, pl.ds(t, heads, stride=tok), :] for b in range(kvh * seq // 128)], axis=1).astype(BF16)
            o_s[pl.ds(t, heads, stride=tok), :] = jnp.dot(pt, vb[t], preferred_element_type=F32)
        pieces = []
        for hh in range(heads):
            sl = slice(hh * tok, (hh + 1) * tok)
            mixed = o_s[sl, :] + w_new[hh].astype(BF16).astype(F32) * v_new[hh // group]
            pieces.append((mixed / den[hh]).astype(BF16))
        o = jnp.concatenate(pieces, axis=1)
        if l == 0:
            with jax.named_scope(f"await5_{l}"):
                attn_copy(l, 5).wait()
            start_up(0, 1)
            start_up(0, 2)
        if l == 0:
            with jax.named_scope("barrier"):
                pl.semaphore_wait(barrier, len(others))
        oc = 256
        for c in range(model // oc):
            sl = slice(c * oc, (c + 1) * oc)
            a = (x[:, sl] + jnp.dot(o, wo_s[:, sl], preferred_element_type=F32)).astype(BF16)
            a_s[:, sl] = a.astype(F32)
            h, at = c * oc // hw, c * oc % hw
            a_all[l, h, me, :, at:at + oc] = a
            if at + oc == hw:
                for k in far_first + (0,):
                    a_copy(l, h, k).start()

    def g_copy(l, j):
        view = g_all.at[l, me]
        return pltpu.make_async_remote_copy(
            src_ref=view, dst_ref=view, send_sem=sem_gs.at[0], recv_sem=sem_g.at[0],
            device_id=peer(*others[j])[1], device_id_type=MESH)

    def wait_all(view, sem):
        pltpu.make_async_copy(view, view, sem).wait()

    def d_copy(l, n, k):
        dest = peer(0, 0, 1)[0] if k == 0 else peer(*chips[k], 0)[0]
        return pltpu.make_async_remote_copy(
            src_ref=part.at[l, n, dest], dst_ref=sbuf.at[l, n, k], send_sem=sem_ds.at[0], recv_sem=sem_d.at[n],
            device_id=peer(0, 0, 1)[1], device_id_type=MESH)

    def c_copy(l, n, k):
        return pltpu.make_async_remote_copy(
            src_ref=red.at[l, n, k], dst_ref=rbuf.at[l, n, k], send_sem=sem_cs.at[0], recv_sem=sem_c.at[n],
            device_id=peer(*chips[k], 1)[1], device_id_type=MESH)

    def route(l):
        u = rms_normed(a_s[...]).astype(BF16)
        if l == 0:
            with jax.named_scope(f"await6_{l}"):
                attn_copy(l, 6).wait()
        rest = wr_s[...]
        n_exp = rest.shape[0]
        logits = jnp.zeros((tok, n_exp), F32)
        for _ in range(3):
            piece = rest.astype(BF16)
            rest = rest - piece.astype(F32)
            logits = logits + lax.dot_general(u, piece, NT, preferred_element_type=F32)
        mine = idt_s[l, pl.ds(row0, tok), :]
        expert = lax.broadcasted_iota(jnp.int32, (tok, n_exp), 1).astype(F32)
        chosen = jnp.zeros((tok, n_exp), jnp.bool_)
        for k in range(mine.shape[1]):
            chosen = chosen | (mine[:, k:k + 1] == expert)
        masked = jnp.where(chosen, logits, -jnp.inf)
        w = jnp.exp(masked - jnp.max(masked, axis=-1, keepdims=True))
        gates = w / jnp.sum(w, axis=-1, keepdims=True)
        g_all[l, me] = jnp.concatenate([gates, jnp.zeros((tok, 128 - n_exp), F32)], axis=1)
        for j in range(len(others)):
            g_copy(l, j).start()

    n_tok = n_dev * tok
    fc = 256

    def up_block(l, lo, hi):
        for i in range(lo, hi):
            ub = u_all[...]
            for n in range(ff // fc):
                sl = slice(n * fc, (n + 1) * fc)
                one = jnp.dot(ub, w1_s[i, :, sl], preferred_element_type=F32)
                three = jnp.dot(ub, w3_s[i, :, sl], preferred_element_type=F32)
                inner_s[i, :, sl] = (jax.nn.silu(one) * three).astype(BF16)

    def gate_columns(l):
        gates = g_all[l].reshape(n_tok, 128)
        first = (ep * n_pool + p) * n_loc
        gates = pltpu.roll(gates, lax.rem(128 - first, 128), 1)
        for i in range(n_loc):
            gb_s[i] = jnp.broadcast_to(gates[:, i:i + 1], (n_tok, 128))

    def down_block(l, n):
        acc = [jnp.zeros((n_tok, 128), F32) for _ in range(cw // 128)]
        for i in range(n_loc):
            y = jnp.dot(inner_s[i], w2_s[n, i], preferred_element_type=F32).astype(BF16).astype(F32)
            g = gb_s[i]
            for b in range(cw // 128):
                acc[b] = acc[b] + jnp.where(g > 0.0, g * y[:, b * 128:(b + 1) * 128], 0.0)
        for b in range(cw // 128):
            part[l, n, :, :, b * 128:(b + 1) * 128] = acc[b].reshape(n_dev, tok, 128)

    def both(l, n):
        return l == layers - 1 and n >= n_chunk - n_both

    def d2_copy(l, n, k):
        dest = peer(*chips[k], 0)[0] if k < 4 else peer(*chips[(k - 4) * 2], 1)[0]
        return pltpu.make_async_remote_copy(
            src_ref=part.at[l, n, dest], dst_ref=sbuf2.at[n - n_chunk + n_both, k], send_sem=sem_ds.at[1], recv_sem=sem_d.at[n],
            device_id=peer(0, 0, 1)[1], device_id_type=MESH)

    def c2_copy(n, k, r):
        m = n - n_chunk + n_both
        return pltpu.make_async_remote_copy(
            src_ref=red2.at[m, (k + 2 * r) % 4], dst_ref=rbuf2.at[m, k, r], send_sem=sem_cs.at[1], recv_sem=sem_c.at[n],
            device_id=peer(*chips[k], 1)[1], device_id_type=MESH)

    def share_chunk(l, n):
        if both(l, n):
            for k in (3, 1, 2, 0, 4, 5):
                d2_copy(l, n, k).start()
        else:
            for k in far_first + (0,):
                d_copy(l, n, k).start()

    def forward_chunk(l, n):
        if both(l, n):
            m = n - n_chunk + n_both
            wait_all(sbuf2.at[m], sem_d.at[n])
            for k in (3, 1, 2, 0):
                red2[m, k] = part[l, n, peer(*chips[k], 1)[0]] + sbuf2[m, k]
                if k == 1:
                    for q in (3, 1):
                        for r in range(2):
                            c2_copy(n, q, r).start()
            for r in range(2):
                c2_copy(n, 2, r).start()
            return
        wait_all(sbuf.at[l, n], sem_d.at[n])
        for k in far_first:
            red[l, n, k] = part[l, n, peer(*chips[k], 1)[0]] + sbuf[l, n, k]
            c_copy(l, n, k).start()

    def up_wait(l, g):
        with jax.named_scope(f"upwait{l}"):
            for c in up_copies(l, g):
                c.wait()

    def experts(l):
        with jax.named_scope(f"uwait{l}"):
            for h in range(2):
                for k in (2, 3, 1):
                    a_arrival(l, h, k).wait()
                    a_relay(l, h, k).start()
        with jax.named_scope(f"urelay{l}"):
            wait_all(a_all.at[l, :, pl.ds(0, 4)], sem_u.at[0])
        for d in range(n_dev):
            v = [a_all[l, h, d].astype(F32) for h in range(2)]
            square = sum(jnp.sum(q * q, axis=-1, keepdims=True) for q in v)
            r = lax.rsqrt(square * (1.0 / model) + EPSILON)
            for h in range(2):
                u_all[d * tok:(d + 1) * tok, h * hw:(h + 1) * hw] = (v[h] * r).astype(BF16)
        n_pair = n_loc // 2
        if l > 0:
            down_copy(l, 0).start()
            down_copy(l, 1).start()
        blocks = (2, 2) if l == 0 else (4,)
        lo = 0
        for gi, step in enumerate(blocks):
            for g in range(lo, lo + step):
                up_wait(l, g)
            if gi == len(blocks) - 1:
                for n in range(2, n_chunk):
                    down_copy(l, n).start()
            elif l == 0:
                for n in range(2):
                    down_copy(l, n).start()
            if gi == 0:
                wait_all(g_all.at[l, pl.ds(0, len(others))], sem_g.at[0])
            with jax.named_scope(f"up{l}"):
                up_block(l, lo * 2, (lo + step) * 2)
                if gi == 0:
                    gate_columns(l)
            lo += step
        for n in range(n_chunk):
            with jax.named_scope(f"downwait{l}"):
                down_copy(l, n).wait()
            if l + 1 < layers:
                if n == 0:
                    for k in range(7):
                        attn_copy(l + 1, k).start()
                else:
                    start_up(l + 1, n - 1)
            with jax.named_scope(f"down{l}"):
                down_block(l, n)
            share_chunk(l, n)
            if n > 0:
                with jax.named_scope(f"fwd{l}"):
                    forward_chunk(l, n - 1)
        if l + 1 < layers:
            start_up(l + 1, n_pair - 1)
        with jax.named_scope(f"fwd{l}"):
            forward_chunk(l, n_chunk - 1)

    other = 1 - p
    orow = pl.multiple_of(other * tok, tok)

    def x_copy(n, row):
        view = xfin.at[pl.ds(row, tok), pl.ds(n * cw, cw)]
        return pltpu.make_async_remote_copy(
            src_ref=view, dst_ref=view, send_sem=sem_x.at[0], recv_sem=sem_x.at[1],
            device_id={"pool": other, "ep": ep}, device_id_type=MESH)

    def combine(l):
        for n in range(n_chunk):
            sl = slice(n * cw, (n + 1) * cw)
            if both(l, n):
                m = n - n_chunk + n_both
                wait_all(rbuf2.at[m, pl.ds(1, 3)], sem_c.at[n])
                ah, at = n * cw // hw, n * cw % hw
                for r in range(2):
                    total = part[l, n, peer(*chips[2 * r], 0)[0]] + sbuf2[m, 4 + r]
                    total = (total + rbuf2[m, 2, r]) + (rbuf2[m, 1, r] + rbuf2[m, 3, r])
                    xfin[pl.ds(orow if r else row0, tok), sl] = (a_all[l, ah, peer(*chips[2 * r], 0)[0], :, at:at + cw].astype(F32) + total).astype(BF16)
                continue
            total = part[l, n, me] + sbuf[l, n, 0]
            wait_all(rbuf.at[l, n, pl.ds(1, 3)], sem_c.at[n])
            total = (total + rbuf[l, n, 2]) + (rbuf[l, n, 1] + rbuf[l, n, 3])
            x = (a_s[:, sl] + total).astype(BF16)
            if l + 1 < layers:
                x_s[:, sl] = x.astype(F32)
            else:
                xfin[pl.ds(row0, tok), sl] = x
                x_copy(n, row0).start()

    for l in range(layers):
        with jax.named_scope(f"attention{l}"):
            attention(l)
        with jax.named_scope(f"route{l}"):
            route(l)
        if l == 0:
            start_up(0, 3)
        experts(l)
        with jax.named_scope(f"combine{l}"):
            combine(l)

    with jax.named_scope("xwait"):
        wait_all(xfin.at[pl.ds(orow, tok), pl.ds(0, model - n_both * cw)], sem_x.at[1])
    with jax.named_scope("drain"):
        wait_all(xfin.at[pl.ds(row0, tok), pl.ds(0, model - n_both * cw)], sem_x.at[0])
        wait_all(a_all.at[:, :, pl.ds(0, 7)], sem_us.at[0])
        wait_all(g_all.at[:, pl.ds(0, 7)], sem_gs.at[0])
        wait_all(part.at[0, pl.ds(0, n_chunk - n_both // 2)], sem_ds.at[0])
        wait_all(part.at[0, pl.ds(0, n_both), pl.ds(0, 6)], sem_ds.at[1])
        wait_all(red.at[:, pl.ds(0, n_chunk - n_both // 2), pl.ds(1, 3)], sem_cs.at[0])
        wait_all(red.at[:, pl.ds(0, n_both), pl.ds(1, 3)], sem_cs.at[1])


def solution(mesh):
    n_pool = mesh.shape["pool"]
    n_ep = mesh.shape["ep"]
    n_dev = n_pool * n_ep

    def body(hidden, k_cache, v_cache, lengths, expert_ids, w_query, w_key, w_value, w_out, w_router, w_gate, w_up, w_down):
        layers, n_tok, seq, kvh, hd = k_cache.shape
        tok = n_tok // n_pool
        model = hidden.shape[1]
        heads = w_query.shape[2] // hd
        n_loc = w_gate.shape[1] // n_pool
        ff = w_gate.shape[3]
        n_exp = w_router.shape[2]
        topk = expert_ids.shape[2]
        cw = 256
        n_chunk = model // cw
        n_both = n_chunk // 2
        kflat = k_cache.reshape(layers, n_tok, seq * kvh, hd)
        vflat = v_cache.reshape(layers, n_tok, seq * kvh, hd)
        ids = jnp.swapaxes(expert_ids, 1, 2)
        router = jnp.swapaxes(w_router, 1, 2)
        cfg = (layers, n_pool, n_ep, tok, heads, kvh, hd, seq, n_loc, ff, model)
        any_spec = pl.BlockSpec(memory_space=pl.ANY)
        vm = pltpu.VMEM
        dma = pltpu.SemaphoreType.DMA
        return pl.pallas_call(
            functools.partial(kernel, cfg),
            out_shape=vm((n_tok, model), BF16),
            in_specs=[any_spec] * 13,
            out_specs=pl.BlockSpec(memory_space=pltpu.VMEM),
            scratch_shapes=[
                vm((model, heads * hd), BF16), vm((model, kvh * hd), BF16), vm((model, kvh * hd), BF16),
                vm((heads * hd, model), BF16), vm((n_exp, model), F32),
                vm((tok, seq * kvh, hd), BF16), vm((tok, seq * kvh, hd), BF16),
                vm((n_loc, model, ff), BF16), vm((n_loc, model, ff), BF16), vm((n_chunk, n_loc, ff, cw), BF16),
                vm((tok, model), F32), vm((tok, model), F32), vm((layers, topk, n_tok), jnp.int32), vm((layers, 128, topk), F32),
                vm((heads * tok, hd), F32), vm((kvh * seq // 128, heads * tok, 128), F32), vm((heads * tok, hd), F32),
                vm((layers, 2, n_dev, tok, model // 2), BF16), vm((n_dev * tok, model), BF16), vm((layers, n_dev, tok, 128), F32), vm((n_loc, n_dev * tok, 128), F32),
                vm((n_loc, n_dev * tok, ff), BF16), vm((layers, n_chunk, n_dev, tok, cw), F32),
                vm((layers, n_chunk, 4, tok, cw), F32), vm((layers, n_chunk, 4, tok, cw), F32), vm((layers, n_chunk, 4, tok, cw), F32),
                vm((n_both, 6, tok, cw), F32), vm((n_both, 4, tok, cw), F32), vm((n_both, 4, 2, tok, cw), F32),
                vm((tok, model), BF16), pltpu.SMEM((n_tok,), jnp.int32),
                dma((10,)), dma((2, n_loc // 2)), dma((n_chunk,)), dma((8,)), dma((1,)), dma((1,)), dma((1,)),
                dma((n_chunk,)), dma((2,)), dma((n_chunk,)), dma((2,)), dma((2,)),
            ],
            compiler_params=pltpu.CompilerParams(
                collective_id=0, has_side_effects=True, vmem_limit_bytes=63 * 1024 * 1024),
        )(hidden, kflat, vflat, lengths, ids, w_query, w_key, w_value, w_out, router, w_gate, w_up, w_down)

    rows_spec = ("dp", "ep")
    in_specs = (P(rows_spec, None), P(None, rows_spec), P(None, rows_spec), P(rows_spec), P(None, rows_spec, None), P(), P(), P(), P(), P(), P(None, "ep"), P(None, "ep"), P(None, "ep"))
    return jax.shard_map(body, mesh=mesh, in_specs=in_specs, out_specs=P(rows_spec, None), check_vma=False)
```
